256 devices in a mesh: dp: 16 (over z, core), ctx: 16 (over x, y).
Axes of the slice: x: 4, y: 4, z: 8, core: 2. Of those that a mesh axis runs over, the one named last changes fastest.
Arguments:
- hidden: bfloat16 [16, 2048, 5120], P('dp', 'ctx'), may hold values from -6 to 6
- queries: bfloat16 [16, 2048, 4096], P('dp', 'ctx'), may hold values from -6 to 6
- key_states: bfloat16 [16, 2048, 512], P('dp', 'ctx'), may hold values from -6 to 6
- out_grad: bfloat16 [16, 2048, 4096], P('dp', 'ctx'), may hold values from -6 to 6
- w_value: bfloat16 [5120, 512], replicated, may hold values from -0.078125 to 0.078125
- q_gain: float32 [128], replicated, may hold values from 0.1 to 1.9
- k_gain: float32 [128], replicated, may hold values from 0.1 to 1.9
- dest_rows: int32 [16, 2048], P('dp', 'ctx'), may hold values from 0 to 2047, as said below
- doc_ids: int32 [16, 2048], P('dp', 'ctx'), may hold values from 0 to 3, never falling along the last dimension, each value on 1 to 1024 neighbouring positions
Outputs:
- hidden_grad: bfloat16 [16, 2048, 5120], P('dp', 'ctx')
- query_grad: bfloat16 [16, 2048, 4096], P('dp', 'ctx')
- key_grad: bfloat16 [16, 2048, 512], P('dp', 'ctx')
- weight_grad: float32 [5120, 512], P(('dp', 'ctx'))
The draws below stay inside these ranges and needn't reach their ends.
Inputs may be any that keep to these rules, and one draw needn't show every extreme that they name: `dest_rows`: within each data group the entries are a permutation of the slab's rows; the 128 entries of one block of arrival rows name exactly 16 or no rows of each block of 128 slab rows. `doc_ids`: ids never fall along a slab.
All inputs are finite; a program needn't handle non-finite values.
Results may differ from the reference program's by a relative error of at most 0.017.
Values may be sent and summed in bfloat16 or wider, within the bound.
A program may use at most 128 MiB of HBM per device.

```python
import math
import jax
import jax.numpy as jnp
import numpy as np
from jax import lax

D = 5120
QH = 32
KVH = 4
HD = 128
TOK_DEV = 128
DOCS = 4
SLAB = 2048
CAP = 16
DOC_MOST = 1024
N_DP = 16
N_CTX = 16


def draw_dest_rows(key, part):

    def arrange(group_key):
        offsets = jax.random.permutation(jax.random.fold_in(group_key, 1), N_CTX)[:N_CTX // 2]
        source_keys = jax.random.split(jax.random.fold_in(group_key, 2), N_CTX)
        target_keys = jax.random.split(jax.random.fold_in(group_key, 3), N_CTX)
        shuffle = jax.vmap(lambda one_key: jax.random.permutation(one_key, TOK_DEV))(source_keys)
        placing = jax.vmap(lambda one_key: jax.random.permutation(one_key, TOK_DEV))(target_keys)
        sources = jnp.arange(N_CTX, dtype=jnp.int32)[:, None]
        owners = (sources + offsets[shuffle // CAP]) % N_CTX
        local_row = placing[owners, shuffle]
        return (owners * TOK_DEV + local_row).reshape(N_CTX * TOK_DEV).astype(jnp.int32)
    group_keys = jax.vmap(lambda group_index: jax.random.fold_in(key, group_index))(jnp.arange(N_DP))
    return jax.vmap(arrange)(group_keys)


def shard_levels(own_key, extent, cuts, smallest, top_value):
    gain = 1.0
    for dim, blocks in cuts:
        heights = jax.random.uniform(jax.random.fold_in(jax.random.fold_in(own_key, 6), dim), (blocks,), jnp.float32, smallest / len(cuts), top_value / len(cuts))
        gain = gain * jnp.repeat(jnp.exp(heights), extent[dim] // blocks).reshape((-1,) + (1,) * (len(extent) - 1 - dim))
    return gain


def split_up(count, total, reach, slope):
    portions = [(1 << 20) // math.isqrt(standing ** slope) + 1 for standing in range(2, count + 1)]
    surplus, counts = total - reach - (count - 1), [1] * (count - 1)
    while surplus > 0:
        free = [i for i in range(count - 1) if counts[i] < reach]
        whole, left = sum([portions[i] for i in free]), surplus
        for i in free:
            extra = min(reach - counts[i], max(1, left * portions[i] // whole), surplus)
            counts[i] = counts[i] + extra
            surplus = surplus - extra
    return np.array([reach] + counts)


def uneven(rng, amount, total, limit, skew):
    if amount == 2:
        one = jax.random.randint(rng, (), max(1, total - limit), min(limit, total - 1) + 1)
        return jnp.stack([one, total - one])
    sizes = jnp.asarray(split_up(amount, total, limit, skew), jnp.int32)
    twos = (amount - 1) // 2
    source_of, taker = sizes[1:1 + 2 * twos:2], sizes[2:2 + 2 * twos:2]
    margin = jnp.minimum(source_of - 1, limit - taker)
    passed = jax.random.randint(jax.random.fold_in(rng, 1), (twos,), 0, 1 << 20) % (margin + 1)
    sizes = sizes.at[1:1 + 2 * twos:2].set(source_of - passed).at[2:2 + 2 * twos:2].set(taker + passed)
    return sizes[jax.random.permutation(jax.random.fold_in(rng, 2), amount)]


def gaussian(rng, extent, width, limit, cuts=(), held_as=jnp.bfloat16):
    entries = width * jax.random.normal(rng, extent, jnp.float32)
    if cuts:
        entries = entries * shard_levels(rng, extent, cuts, -0.22, 0.18)
    return jnp.clip(entries, -limit, limit).astype(held_as)


def setup_inputs(seed: int = 0) -> dict:
    keys = jax.random.split(jax.random.key(seed), 10)
    return {
        "hidden": gaussian(keys[0], (N_DP, SLAB, D), 1.0, 6.0, ((0, 16), (1, 16))),
        "queries": gaussian(keys[1], (N_DP, SLAB, QH * HD), 1.0, 6.0, ((0, 16), (1, 16))),
        "key_states": gaussian(keys[2], (N_DP, SLAB, KVH * HD), 1.0, 6.0, ((0, 16), (1, 16))),
        "out_grad": gaussian(keys[3], (N_DP, SLAB, QH * HD), 1.0, 6.0, ((0, 16), (1, 16))),
        "w_value": gaussian(keys[4], (D, KVH * HD), D ** -0.5, 0.078125),
        "q_gain": jnp.clip(1.0 + 0.18 * jax.random.normal(keys[5], (HD,), jnp.float32), 0.1, 1.9),
        "k_gain": jnp.clip(1.0 + 0.18 * jax.random.normal(keys[6], (HD,), jnp.float32), 0.1, 1.9),
        "dest_rows": draw_dest_rows(jax.random.fold_in(keys[9], 71), 0),
        "doc_ids": jax.vmap(lambda own: jnp.searchsorted(jnp.cumsum(uneven(own, DOCS, SLAB, DOC_MOST, 2)), jnp.arange(SLAB), side="right"))(jax.random.split(keys[8], N_DP)).reshape((N_DP, SLAB)).astype(jnp.int32),
    }


epsilon = 1e-06
rope_base = 1000000.0
highest = lax.Precision.HIGHEST

def rounded(array):
    return lax.optimization_barrier(array.astype(jnp.bfloat16)).astype(jnp.float32)

def doc_positions(doc_ids):
    position_index = jnp.arange(doc_ids.shape[0], dtype=jnp.int32)
    change = jnp.concatenate([jnp.ones((1,), dtype=bool), doc_ids[1:] != doc_ids[:-1]])
    starts = lax.cummax(jnp.where(change, position_index, 0).astype(jnp.int32), axis=0)
    return position_index - starts

def rope_tables(positions, head_width):
    half_width = head_width // 2
    frequency = rope_base ** (-(jnp.arange(half_width, dtype=jnp.float32) * 2.0 / head_width))
    angles = positions.astype(jnp.float32)[:, None] * frequency[None, :]
    return (jnp.cos(angles), jnp.sin(angles))

def norm_rope(vector, gain_vector, cosine, sine_table):
    inverse_rms = lax.rsqrt(lax.optimization_barrier(jnp.mean(vector * vector, axis=-1, keepdims=True)) + epsilon)
    normed = vector * inverse_rms * gain_vector
    half_width = vector.shape[-1] // 2
    first_half = normed[..., :half_width]
    second_half = normed[..., half_width:]
    cos_rows = cosine[:, None, :]
    sin_rows = sine_table[:, None, :]
    return jnp.concatenate([first_half * cos_rows - second_half * sin_rows, second_half * cos_rows + first_half * sin_rows], axis=-1)

def head_set(q_set, k_head, v_head, g_set, doc_ids, cosine, sine_table, q_gain, k_gain):
    q_normed, q_back = jax.vjp(lambda operand: norm_rope(operand, q_gain, cosine, sine_table), q_set.astype(jnp.float32))
    k_normed, k_back = jax.vjp(lambda operand: norm_rope(operand, k_gain, cosine, sine_table), k_head.astype(jnp.float32))
    q_values = rounded(q_normed)
    k_values = rounded(k_normed)[:, 0]
    v_values = v_head.astype(jnp.float32)
    g_values = g_set.astype(jnp.float32)
    factor = q_set.shape[2] ** (-0.5)
    position_index = jnp.arange(q_set.shape[0], dtype=jnp.int32)
    allowed = (doc_ids[:, None] == doc_ids[None, :]) & (position_index[:, None] >= position_index[None, :])
    logits = jnp.einsum('qhd,kd->hqk', q_values, k_values, precision=highest) * factor
    exponent = jnp.where(allowed[None], jnp.exp(logits), 0.0)
    denominator = lax.optimization_barrier(jnp.sum(exponent, axis=-1))
    outputs = jnp.einsum('hqk,kd->hqd', rounded(exponent), v_values, precision=highest) / denominator[..., None]
    probability = exponent / denominator[..., None]
    delta_row = lax.optimization_barrier(jnp.sum(jnp.swapaxes(g_values, 0, 1) * outputs, axis=-1))
    prob_grad = jnp.einsum('qhd,kd->hqk', g_values, v_values, precision=highest)
    dlogit = rounded(probability * (prob_grad - delta_row[..., None]))
    q_grad = jnp.einsum('hqk,kd->qhd', dlogit, k_values, precision=highest) * factor
    k_grad = jnp.einsum('hqk,qhd->kd', dlogit, q_values, precision=highest) * factor
    v_grad = jnp.einsum('hqk,qhd->kd', rounded(probability), g_values, precision=highest)
    q_pre = q_back(q_grad)[0].astype(jnp.bfloat16)
    k_pre = k_back(k_grad[:, None, :])[0][:, 0].astype(jnp.bfloat16)
    return (q_pre, jnp.concatenate([k_pre, v_grad.astype(jnp.bfloat16)], axis=-1))

def one_group(hidden, queries, key_states, out_grad, dest_rows, doc_ids, w_value, q_gain, k_gain):
    slab_rows = hidden.shape[0]
    head_width = q_gain.shape[0]
    kv_count = key_states.shape[1] // head_width
    set_heads = queries.shape[1] // (N_CTX * head_width)
    share_count = N_CTX // kv_count
    balanced = jnp.zeros_like(hidden).at[dest_rows.astype(jnp.int32)].set(hidden)
    value_rows = jnp.dot(balanced, w_value, preferred_element_type=jnp.float32).astype(jnp.bfloat16)
    cosine, sine_table = rope_tables(doc_positions(doc_ids), head_width)
    q_sets = queries.reshape(slab_rows, N_CTX, set_heads, head_width)
    g_sets = out_grad.reshape(slab_rows, N_CTX, set_heads, head_width)
    k_heads = key_states.reshape(slab_rows, kv_count, head_width)
    v_heads = value_rows.reshape(slab_rows, kv_count, head_width)

    def per_set(set_index):
        head_index = set_index // share_count
        q_set = lax.dynamic_index_in_dim(q_sets, set_index, axis=1, keepdims=False)
        g_set = lax.dynamic_index_in_dim(g_sets, set_index, axis=1, keepdims=False)
        k_head = lax.dynamic_slice_in_dim(k_heads, head_index, 1, axis=1)
        v_head = lax.dynamic_index_in_dim(v_heads, head_index, axis=1, keepdims=False)
        return head_set(q_set, k_head, v_head, g_set, doc_ids, cosine, sine_table, q_gain, k_gain)
    q_parts, kv_parts = lax.map(per_set, jnp.arange(N_CTX, dtype=jnp.int32))
    query_grad = jnp.transpose(q_parts, (1, 0, 2, 3)).reshape(slab_rows, N_CTX * set_heads * head_width)
    summed = kv_parts.astype(jnp.float32).reshape(kv_count, share_count, slab_rows, 2 * head_width).sum(axis=1)
    summed = jnp.transpose(summed, (1, 0, 2))
    key_grad = summed[..., :head_width].astype(jnp.bfloat16).reshape(slab_rows, kv_count * head_width)
    value_grad = summed[..., head_width:].astype(jnp.bfloat16).reshape(slab_rows, kv_count * head_width)
    hidden_grad = jnp.dot(value_grad, w_value.T, preferred_element_type=jnp.float32).astype(jnp.bfloat16)
    weight_part = jnp.dot(balanced.T, value_grad, preferred_element_type=jnp.float32)
    return (hidden_grad, query_grad, key_grad, weight_part)

def reference(hidden, queries, key_states, out_grad, w_value, q_gain, k_gain, dest_rows, doc_ids):

    def accumulate(total, group):
        hidden_grad, query_grad, key_grad, weight_part = one_group(*group, w_value, q_gain, k_gain)
        return (total + weight_part, (hidden_grad, query_grad, key_grad))
    start = jnp.zeros((D, KVH * HD), dtype=jnp.float32)
    total, (hidden_grad, query_grad, key_grad) = lax.scan(accumulate, start, (hidden, queries, key_states, out_grad, dest_rows, doc_ids))
    weight_grad = total / (N_DP * N_CTX)
    return (hidden_grad, query_grad, key_grad, weight_grad)
```

```python
import functools
import math

import jax
import jax.numpy as jnp
import numpy as np
from jax import lax
from jax.experimental import pallas as pl
from jax.experimental.pallas import tpu as pltpu
from jax.sharding import PartitionSpec as P

epsilon = 1e-06
rope_base = 1000000.0
BF16, F32, I32 = jnp.bfloat16, jnp.float32, jnp.int32
ANY = pl.BlockSpec(memory_space=pl.ANY)
VMEM = pl.BlockSpec(memory_space=pltpu.VMEM)
TILE = 256
NT = (((1,), (1,)), ((), ()))
TN = (((0,), (0,)), ((), ()))


def dot(a, b, dims=(((1,), (0,)), ((), ()))):
    return lax.dot_general(a, b, dims, preferred_element_type=F32)


def send(src, dst, ssem, rsem, dp, ctx):
    return pltpu.make_async_remote_copy(
        src_ref=src,
        dst_ref=dst,
        send_sem=ssem,
        recv_sem=rsem,
        device_id=(dp, ctx),
        device_id_type=pl.DeviceIdType.MESH,
    )


def signal(sem, dp, ctx):
    pl.semaphore_signal(
        sem, inc=1, device_id=(dp, ctx), device_id_type=pl.DeviceIdType.MESH
    )


def window(dp, share):
    return pl.multiple_of((dp * share) // 128 * 128, 128)


def arrive_kernel(
    sizes, q, g, k, h, w, index, q_o, g_o, k_o, v_o, index_o, hf_o,
    h_v, w_v, v_v, ssem, rsem, hssem, hrsem, lsem,
):
    n_dp, n_ctx, rows, width, head, per_kv, share, win = sizes
    dp, me = lax.axis_index("dp"), lax.axis_index("ctx")

    load_h = pltpu.make_async_copy(h, h_v, lsem.at[6])
    load_w = pltpu.make_async_copy(w, w_v, lsem.at[7])
    load_h.start()
    load_w.start()

    barrier = pltpu.get_barrier_semaphore()

    @pl.loop(1, n_ctx)
    def _(d):
        signal(barrier, dp, lax.rem(me + d, n_ctx))

    @pl.loop(1, n_dp)
    def _(d):
        signal(barrier, lax.rem(dp + d, n_dp), me)

    pl.semaphore_wait(barrier, n_ctx - 1 + n_dp - 1)

    def cols(s, size):
        return pl.ds(pl.multiple_of(s * size, size), size)

    def block(c):
        return pl.ds(pl.multiple_of(c * rows, rows), rows)

    def pieces(to, frm):
        return (
            (index, index_o.at[frm]),
            (k.at[:, cols(to // per_kv, head)], k_o.at[block(frm), :]),
            (q.at[:, cols(to, width)], q_o.at[block(frm), :]),
            (g.at[:, cols(to, width)], g_o.at[block(frm), :]),
            (v_v.at[:, cols(to // per_kv, head)], v_o.at[block(frm), :]),
        )

    def ctx_copy(kind, d, to, frm):
        src, dst = pieces(to, frm)[kind]
        return send(src, dst, ssem.at[kind, d], rsem.at[kind, d], dp, to)

    def hf_copy(d, to, frm):
        return send(
            h_v.at[:, pl.ds(window(to, share), win)],
            hf_o.at[frm],
            hssem.at[d],
            hrsem.at[d],
            to,
            me,
        )

    for kind in range(4):

        @pl.loop(1, n_ctx)
        def _(d, kind=kind):
            ctx_copy(kind, d, lax.rem(me + d, n_ctx), me).start()

    local = [
        pltpu.make_async_copy(src, dst, lsem.at[i])
        for i, (src, dst) in enumerate(pieces(me, me)[:4])
    ]
    for copy in local:
        copy.start()
    load_h.wait()

    @pl.loop(1, n_dp)
    def _(d):
        hf_copy(d, lax.rem(dp + d, n_dp), dp).start()

    own_hf = pltpu.make_async_copy(
        h_v.at[:, pl.ds(window(dp, share), win)], hf_o.at[dp], lsem.at[5]
    )
    own_hf.start()
    load_w.wait()
    v_v[...] = dot(h_v[...], w_v[...]).astype(BF16)

    @pl.loop(1, n_ctx)
    def _(d):
        ctx_copy(4, d, lax.rem(me + d, n_ctx), me).start()

    src, dst = pieces(me, me)[4]
    own_v = pltpu.make_async_copy(src, dst, lsem.at[4])
    own_v.start()
    for copy in local:
        copy.wait()
    own_hf.wait()
    own_v.wait()
    for kind in range(5):

        @pl.loop(1, n_ctx)
        def _(d, kind=kind):
            ctx_copy(kind, d, lax.rem(me + d, n_ctx), me).wait_send()
            frm = lax.rem(me + n_ctx - d, n_ctx)
            ctx_copy(kind, d, me, frm).wait_recv()

    @pl.loop(1, n_dp)
    def _(d):
        hf_copy(d, lax.rem(dp + d, n_dp), dp).wait_send()
        frm = lax.rem(dp + n_dp - d, n_dp)
        hf_copy(d, dp, frm).wait_recv()


def attend_kernel(
    sizes, q_ref, g_ref, k_ref, v_ref, dest_ref, ids_ref, qg_ref, kg_ref, fr_ref, clo_ref, slo_ref,
    gq_ref, gk_ref, gv_ref, ga_ref,
    qs, gs, kn, vs, cs, sn, es, ds_, gk_acc, gv_acc,
):
    slab, heads, head, n_docs = sizes
    tiles = slab // TILE
    factor = head ** (-0.5)
    half = head // 2

    ids = ids_ref[...]
    counts = [jnp.sum((ids < d).astype(F32)) for d in range(1, n_docs)]
    bounds = [c.astype(I32) for c in counts]

    def start_of(row):
        start = jnp.zeros_like(row)
        for b in bounds:
            start = jnp.where(row >= b, b, start)
        return start

    q_gain = qg_ref[...]
    k_gain = kg_ref[...]
    lane = lax.broadcasted_iota(I32, (1, head), 1)
    sign = jnp.where(lane < half, -1.0, 1.0).astype(F32)

    def normrope(u, gain, c, s):
        inv = lax.rsqrt(jnp.mean(u * u, axis=-1, keepdims=True) + epsilon)
        y = u * inv * gain
        return y * c + pltpu.roll(y, half, 1) * s

    def normrope_back(u, gz, gain, c, s):
        inv = lax.rsqrt(jnp.mean(u * u, axis=-1, keepdims=True) + epsilon)
        hat = u * inv
        gn = (gz * c - pltpu.roll(gz, half, 1) * s) * gain
        return inv * (gn - hat * jnp.mean(gn * hat, axis=-1, keepdims=True))

    @pl.loop(0, tiles)
    def _(i):
        r0 = pl.multiple_of(i * TILE, TILE)
        at = pl.ds(r0, TILE)
        row = lax.broadcasted_iota(I32, (TILE, 1), 0) + r0
        base = [jnp.zeros((), I32)] + bounds
        c0 = s0 = None
        for d, b in enumerate(base):
            angle = (r0 - b).astype(F32) * fr_ref[...]
            c_d, s_d = jnp.cos(angle)[:1], jnp.sin(angle)[:1]
            if d == 0:
                c0 = jnp.broadcast_to(c_d, (TILE, head))
                s0 = jnp.broadcast_to(s_d, (TILE, head))
            else:
                c0 = jnp.where(row >= b, c_d, c0)
                s0 = jnp.where(row >= b, s_d, s0)
        clo, slo = clo_ref[...], slo_ref[...]
        c = clo * c0 - slo * s0
        s = (slo * c0 + clo * s0) * sign
        cs[at, :] = c
        sn[at, :] = s
        for hd in range(heads):
            lanes = slice(hd * head, (hd + 1) * head)
            to = slice(hd * TILE, (hd + 1) * TILE)
            u = q_ref[at, lanes].astype(F32)
            qs[i, to, :] = normrope(u, q_gain, c, s).astype(BF16)
            gs[i, to, :] = g_ref[at, lanes]
        kn[at, :] = normrope(k_ref[at, :].astype(F32), k_gain, c, s).astype(BF16)
        gk_acc[at, :] = jnp.zeros((TILE, head), F32)
        gv_acc[at, :] = jnp.zeros((TILE, head), F32)

    def placing(i):
        row = lax.broadcasted_iota(I32, (TILE, 1), 0) + i * TILE
        return jnp.where(row == dest_ref[...], 1.0, 0.0).astype(BF16)

    @pl.loop(0, tiles)
    def _(i):
        r0 = pl.multiple_of(i * TILE, TILE)
        vs[pl.ds(r0, TILE), :] = dot(placing(i), v_ref[...]).astype(BF16)

    scale = factor * math.log2(math.e)

    @pl.loop(0, tiles)
    def _(i):
        r0 = pl.multiple_of(i * TILE, TILE)
        row = lax.broadcasted_iota(I32, (1, TILE), 1) + r0
        start = start_of(row)
        first = jnp.zeros((), I32)
        for b in bounds:
            first = jnp.where(r0 >= b, b, first)
        low = first // TILE
        qi, gi = qs[i], gs[i]

        def forward(j, carry):
            total, num = carry
            k0 = pl.multiple_of(j * TILE, TILE)
            at = pl.ds(k0, TILE)
            key = lax.broadcasted_iota(I32, (TILE, 1), 0) + k0
            allowed = (key >= start) & (key <= row)
            logits = dot(kn[at, :], qi, NT) * scale
            pg = dot(vs[at, :], gi, NT)
            es_parts = []
            for hd in range(heads):
                lanes = slice(hd * TILE, (hd + 1) * TILE)
                es_parts.append(jnp.where(allowed, jnp.exp2(logits[:, lanes]), 0.0))
            e = jnp.concatenate(es_parts, axis=1)
            es[j] = e
            ds_[j] = pg
            total = total + jnp.sum(e, axis=0, keepdims=True)
            num = num + jnp.sum(e * pg, axis=0, keepdims=True)
            return total, num

        zero = jnp.zeros((1, heads * TILE), F32)
        total, num = lax.fori_loop(low, i + 1, forward, (zero, zero))
        inv = 1.0 / total
        delta = num * inv

        def backward(j, acc):
            at = pl.ds(pl.multiple_of(j * TILE, TILE), TILE)
            p = es[j] * inv
            dsj = (p * (ds_[j] - delta)).astype(BF16)
            gk_acc[at, :] += dot(dsj, qi)
            gv_acc[at, :] += dot(p.astype(BF16), gi)
            return acc + dot(dsj, kn[at, :], TN)

        acc = lax.fori_loop(low, i + 1, backward, jnp.zeros((heads * TILE, head), F32))
        at = pl.ds(r0, TILE)
        for hd in range(heads):
            lanes = slice(hd * head, (hd + 1) * head)
            gz = acc[hd * TILE : (hd + 1) * TILE] * factor
            u = q_ref[at, lanes].astype(F32)
            gq_ref[at, lanes] = normrope_back(u, gz, q_gain, cs[at, :], sn[at, :]).astype(BF16)

    @pl.loop(0, tiles)
    def _(i):
        at = pl.ds(pl.multiple_of(i * TILE, TILE), TILE)
        gz = gk_acc[at, :] * factor
        u = k_ref[at, :].astype(F32)
        gk_ref[at, :] = normrope_back(u, gz, k_gain, cs[at, :], sn[at, :]).astype(BF16)
        gv_ref[at, :] = gv_acc[at, :].astype(BF16)
        gv_acc[at, :] = jnp.zeros((TILE, head), F32)

    @pl.loop(0, tiles)
    def _(i):
        at = pl.ds(pl.multiple_of(i * TILE, TILE), TILE)
        gv_acc[...] += dot(placing(i), gv_ref[at, :], TN)

    ga_ref[...] = gv_acc[...].astype(BF16)


def return_kernel(
    sizes, gq, gk, gv, ga, w, hf, gq_o, gk_o, h_o, w_o,
    kr, vr, ar, vg, ag, w_v, hf_v, dw, dws, dwr,
    ssem, rsem, lsem, ag_s, ag_r, ws, wr,
):
    n_dp, n_ctx, rows, width, head, per_kv, share, win = sizes
    n_z = n_dp // 2
    dp, me = lax.axis_index("dp"), lax.axis_index("ctx")
    z, core = dp // 2, dp % 2
    after = lax.rem(z + 1, n_z) * 2 + core
    before = lax.rem(z + n_z - 1, n_z) * 2 + core
    twin = z * 2 + 1 - core
    ahead = n_z // 2
    behind = n_z - 1 - ahead
    kv = n_ctx // per_kv

    load_w = pltpu.make_async_copy(w, w_v, lsem.at[4])
    load_hf = pltpu.make_async_copy(hf, hf_v, lsem.at[5])
    load_w.start()
    load_hf.start()

    barrier = pltpu.get_barrier_semaphore()

    @pl.loop(1, n_ctx)
    def _(d):
        signal(barrier, dp, lax.rem(me + d, n_ctx))

    around = [after, before, twin] if n_z > 2 else ([after, twin] if n_z > 1 else [twin])
    for other in around:
        signal(barrier, other, me)
    pl.semaphore_wait(barrier, n_ctx - 1 + len(around))

    def block(c):
        return pl.ds(pl.multiple_of(c * rows, rows), rows)

    def pieces(to, frm):
        place = pl.ds(pl.multiple_of(frm * width, width), width)
        return (
            (ga.at[block(to), :], ar.at[frm]),
            (gv.at[block(to), :], vr.at[frm]),
            (gk.at[block(to), :], kr.at[frm]),
            (gq.at[block(to), :], gq_o.at[:, place]),
        )

    def ctx_copy(kind, d, to, frm):
        src, dst = pieces(to, frm)[kind]
        return send(src, dst, ssem.at[kind, d], rsem.at[kind, d], dp, to)

    local = []
    for kind in range(4):

        @pl.loop(1, n_ctx)
        def _(d, kind=kind):
            ctx_copy(kind, d, lax.rem(me + d, n_ctx), me).start()

        src, dst = pieces(me, me)[kind]
        local.append(pltpu.make_async_copy(src, dst, lsem.at[kind]))
        local[-1].start()

    def arrived(kind):
        local[kind].wait()

        @pl.loop(1, n_ctx)
        def _(d):
            ctx_copy(kind, d, me, lax.rem(me + n_ctx - d, n_ctx)).wait_recv()

    def sums(ref, head_index):
        total = ref[head_index * per_kv].astype(F32)
        for s in range(1, per_kv):
            total = total + ref[head_index * per_kv + s].astype(F32)
        return total.astype(BF16)

    arrived(0)
    for hd in range(kv):
        ag[dp, :, hd * head : (hd + 1) * head] = sums(ar, hd)
    chunk = kv * head // 2

    def part(slot, ch):
        return ag.at[slot, :, pl.ds(ch * chunk, chunk)]

    def ring(slot, ch, way, to):
        return send(part(slot, ch), part(slot, ch), ag_s.at[slot, way, ch], ag_r.at[slot, ch], to, me)

    sent = []

    def go(slot, ch, way, to):
        copy = ring(slot, ch, way, to)
        copy.start()
        sent.append(copy)

    for ch in range(2):
        if ahead:
            go(dp, ch, 0, after)
        if behind:
            go(dp, ch, 1, before)
    for ch in range(2):
        go(dp, ch, 2, twin)

    load_w.wait()
    arrived(1)
    for hd in range(kv):
        vg[:, hd * head : (hd + 1) * head] = sums(vr, hd)

    model = h_o.shape[1]
    steps = max(ahead, 1)
    piece = model // steps
    sub = 256 if piece % 256 == 0 else piece
    for t in range(1, steps + 1):

        @pl.loop(0, piece // sub)
        def _(n, t=t):
            at = pl.ds(pl.multiple_of((t - 1) * piece + n * sub, sub), sub)
            h_o[:, at] = dot(vg[...], w_v[at, :], NT).astype(BF16)

        for ch in range(2):
            if t <= ahead:
                slot = lax.rem(z + n_z - t, n_z) * 2 + core
                ring(slot, ch, 0, after).wait_recv()
                if t < ahead:
                    go(slot, ch, 0, after)
                go(slot, ch, 2, twin)
            if t <= behind:
                slot = lax.rem(z + t, n_z) * 2 + core
                ring(slot, ch, 1, before).wait_recv()
                if t < behind:
                    go(slot, ch, 1, before)
                go(slot, ch, 2, twin)

    arrived(2)
    for hd in range(kv):
        gk_o[:, hd * head : (hd + 1) * head] = sums(kr, hd)
    for t in range(n_z):
        slot = lax.rem(z + t, n_z) * 2 + 1 - core
        for ch in range(2):
            ring(slot, ch, 2, twin).wait_recv()

    load_hf.wait()
    group = 4

    for n in range(n_dp // group):
        at = slice(n * group, (n + 1) * group)
        a = hf_v[at].reshape(group * rows, win)
        b = ag[at].reshape(group * rows, kv * head)
        part_sum = dot(a, b, TN)
        if n == 0:
            dw[...] = part_sum
        else:
            dw[...] += part_sum
    off = pl.multiple_of(dp * share - (dp * share) // 128 * 128, 64)
    out_rows = share // n_ctx
    pad = dws.shape[1]
    for c in range(n_ctx):
        dws[c, :out_rows, :] = dw[pl.ds(off, share), :][c * out_rows : (c + 1) * out_rows].astype(BF16)
        if pad > out_rows:
            dws[c, out_rows:, :] = jnp.zeros((pad - out_rows, kv * head), BF16)

    def w_copy(d, to, frm):
        return send(dws.at[to], dwr.at[frm], ws.at[d], wr.at[d], dp, to)

    @pl.loop(1, n_ctx)
    def _(d):
        w_copy(d, lax.rem(me + d, n_ctx), me).start()

    dwr[me] = dws[me]

    @pl.loop(1, n_ctx)
    def _(d):
        w_copy(d, me, lax.rem(me + n_ctx - d, n_ctx)).wait_recv()

    total = dwr[0].astype(F32)
    for c in range(1, n_ctx):
        total = total + dwr[c].astype(F32)
    w_o[...] = total[:out_rows] * (1.0 / (n_dp * n_ctx))

    arrived(3)
    for copy in sent:
        copy.wait_send()
    for kind in range(4):

        @pl.loop(1, n_ctx)
        def _(d, kind=kind):
            ctx_copy(kind, d, lax.rem(me + d, n_ctx), me).wait_send()

    @pl.loop(1, n_ctx)
    def _(d):
        w_copy(d, lax.rem(me + d, n_ctx), me).wait_send()


def on_device(hidden, queries, key_states, out_grad, w_value, q_gain, k_gain, dest_rows, doc_ids):
    n_dp, n_ctx = lax.axis_size("dp"), lax.axis_size("ctx")
    rows, model = hidden.shape[1:]
    head = q_gain.shape[0]
    kv_width = key_states.shape[2]
    kv = kv_width // head
    width = queries.shape[2] // n_ctx
    heads = width // head
    per_kv = n_ctx // kv
    slab = rows * n_ctx
    share = model // n_dp
    win = (share + 127) // 128 * 128
    sizes = (n_dp, n_ctx, rows, width, head, per_kv, share, win)
    sds = jax.ShapeDtypeStruct
    dma = pltpu.SemaphoreType.DMA

    index = jnp.concatenate([dest_rows, doc_ids], axis=0)
    q_in, g_in, k_in, v_in, index_in, hf = pl.pallas_call(
        functools.partial(arrive_kernel, sizes),
        out_shape=(
            sds((slab, width), BF16),
            sds((slab, width), BF16),
            sds((slab, head), BF16),
            sds((slab, head), BF16),
            sds((n_ctx, 2, rows), I32),
            sds((n_dp, rows, win), BF16),
        ),
        in_specs=[ANY] * 6,
        out_specs=(ANY,) * 6,
        scratch_shapes=[
            pltpu.VMEM((rows, model), BF16),
            pltpu.VMEM((model, kv_width), BF16),
            pltpu.VMEM((rows, kv_width), BF16),
            dma((5, n_ctx)),
            dma((5, n_ctx)),
            dma((n_dp,)),
            dma((n_dp,)),
            dma((8,)),
        ],
        compiler_params=pltpu.CompilerParams(
            collective_id=0, has_side_effects=True, vmem_limit_bytes=32 << 20
        ),
        name="arrive",
    )(queries[0], out_grad[0], key_states[0], hidden[0], w_value, index)

    dest_all = index_in[:, 0].reshape(1, slab)
    ids_all = index_in[:, 1]
    half = head // 2
    frequency = rope_base ** (-(np.arange(half, dtype=np.float64) * 2.0 / head))
    frequency = np.concatenate([frequency, frequency])[None]
    low = np.arange(TILE, dtype=np.float64)[:, None] * frequency
    consts = [
        jnp.asarray(np.broadcast_to(frequency, (8, head)), F32),
        jnp.asarray(np.cos(low), F32),
        jnp.asarray(np.sin(low), F32),
    ]
    tiles = slab // TILE
    gq, gk, gv, ga = pl.pallas_call(
        functools.partial(attend_kernel, (slab, heads, head, 4)),
        out_shape=(
            sds((slab, width), BF16),
            sds((slab, head), BF16),
            sds((slab, head), BF16),
            sds((slab, head), BF16),
        ),
        in_specs=[VMEM] * 11,
        out_specs=(VMEM,) * 4,
        scratch_shapes=[
            pltpu.VMEM((tiles, heads * TILE, head), BF16),
            pltpu.VMEM((tiles, heads * TILE, head), BF16),
            pltpu.VMEM((slab, head), BF16),
            pltpu.VMEM((slab, head), BF16),
            pltpu.VMEM((slab, head), F32),
            pltpu.VMEM((slab, head), F32),
            pltpu.VMEM((tiles, TILE, heads * TILE), F32),
            pltpu.VMEM((tiles, TILE, heads * TILE), F32),
            pltpu.VMEM((slab, head), F32),
            pltpu.VMEM((slab, head), F32),
        ],
        compiler_params=pltpu.CompilerParams(vmem_limit_bytes=48 << 20),
        name="attend",
    )(q_in, g_in, k_in, v_in, dest_all, ids_all, q_gain[None], k_gain[None], *consts)

    out_rows = share // n_ctx
    pad = (out_rows + 15) // 16 * 16
    query_grad, key_grad, hidden_grad, weight_grad = pl.pallas_call(
        functools.partial(return_kernel, sizes),
        out_shape=(
            sds((rows, n_ctx * width), BF16),
            sds((rows, kv_width), BF16),
            sds((rows, model), BF16),
            sds((out_rows, kv_width), F32),
        ),
        in_specs=[ANY] * 6,
        out_specs=(ANY, VMEM, VMEM, VMEM),
        scratch_shapes=[
            pltpu.VMEM((n_ctx, rows, head), BF16),
            pltpu.VMEM((n_ctx, rows, head), BF16),
            pltpu.VMEM((n_ctx, rows, head), BF16),
            pltpu.VMEM((rows, kv_width), BF16),
            pltpu.VMEM((n_dp, rows, kv_width), BF16),
            pltpu.VMEM((model, kv_width), BF16),
            pltpu.VMEM((n_dp, rows, win), BF16),
            pltpu.VMEM((win, kv_width), F32),
            pltpu.VMEM((n_ctx, pad, kv_width), BF16),
            pltpu.VMEM((n_ctx, pad, kv_width), BF16),
            dma((4, n_ctx)),
            dma((4, n_ctx)),
            dma((6,)),
            dma((n_dp, 3, 2)),
            dma((n_dp, 2)),
            dma((n_ctx,)),
            dma((n_ctx,)),
        ],
        compiler_params=pltpu.CompilerParams(
            collective_id=1, has_side_effects=True, vmem_limit_bytes=32 << 20
        ),
        name="give_back",
    )(gq, gk, gv, ga, w_value, hf)
    return (hidden_grad[None], query_grad[None], key_grad[None], weight_grad)


def solution(mesh):
    rows = P("dp", "ctx", None)
    return jax.shard_map(
        on_device,
        mesh=mesh,
        in_specs=(rows, rows, rows, rows, P(), P(), P(), P("dp", "ctx"), P("dp", "ctx")),
        out_specs=(rows, rows, rows, P(("dp", "ctx"), None)),
        check_vma=False,
    )
```

```python
import functools
import math

import jax
import jax.numpy as jnp
import numpy as np
from jax import lax
from jax.experimental import pallas as pl
from jax.experimental.pallas import tpu as pltpu
from jax.sharding import PartitionSpec as P

epsilon = 1e-06
rope_base = 1000000.0
BF16, F32, I32 = jnp.bfloat16, jnp.float32, jnp.int32
ANY = pl.BlockSpec(memory_space=pl.ANY)
HBM = pl.BlockSpec(memory_space=pltpu.HBM)
VMEM = pl.BlockSpec(memory_space=pltpu.VMEM)
TILE = 256
NT = (((1,), (1,)), ((), ()))
TN = (((0,), (0,)), ((), ()))


def dot(a, b, dims=(((1,), (0,)), ((), ()))):
    return lax.dot_general(a, b, dims, preferred_element_type=F32)


def send(src, dst, ssem, rsem, dp, ctx):
    return pltpu.make_async_remote_copy(
        src_ref=src,
        dst_ref=dst,
        send_sem=ssem,
        recv_sem=rsem,
        device_id=(dp, ctx),
        device_id_type=pl.DeviceIdType.MESH,
    )


def signal(sem, dp, ctx):
    pl.semaphore_signal(
        sem, inc=1, device_id=(dp, ctx), device_id_type=pl.DeviceIdType.MESH
    )


def window(dp, share):
    return pl.multiple_of((dp * share) // 128 * 128, 128)


def far(d, n_z):
    return n_z == 8 and d in (3, 5)


def arrive_kernel(
    sizes, q, g, k, h, w, index, q_o, g_o, k_o, v_o, index_o, hf_o,
    h_v, w_v, v_v, ssem, rsem, ysem, yrem, isem, irem, hssem, hrsem, lsem,
):
    n_dp, n_x, n_y, rows, width, head, share, win = sizes
    n_ctx, n_z = n_x * n_y, n_dp // 2
    dp, me = lax.axis_index("dp"), lax.axis_index("ctx")
    x, y, z, core = me // n_y, me % n_y, dp // 2, dp % 2

    load_h = pltpu.make_async_copy(h, h_v, lsem.at[0])
    load_w = pltpu.make_async_copy(w, w_v, lsem.at[1])
    load_h.start()
    load_w.start()

    barrier = pltpu.get_barrier_semaphore()

    @pl.loop(1, n_ctx)
    def _(d):
        signal(barrier, dp, lax.rem(me + d, n_ctx))

    @pl.loop(1, n_dp)
    def _(d):
        signal(barrier, lax.rem(dp + d, n_dp), me)

    pl.semaphore_wait(barrier, n_ctx - 1 + n_dp - 1)

    def cols(s, size):
        return pl.ds(pl.multiple_of(s * size, size), size)

    def on_x(kind, d, to, frm):
        src, dst = (
            (k.at[:, cols(to, head)], k_o.at[y, frm]),
            (q.at[:, cols(to, width)], q_o.at[frm]),
            (v_v.at[:, cols(to, head)], v_o.at[y, frm]),
            (g.at[:, cols(to, width)], g_o.at[frm]),
        )[kind]
        if d == 0:
            return pltpu.make_async_copy(src, dst, lsem.at[2 + kind])
        return send(src, dst, ssem.at[kind, d], rsem.at[kind, d], dp, to * n_y + y)

    def on_y(kind, d, to, frm):
        ref = (k_o, v_o)[kind]
        return send(ref.at[frm], ref.at[frm], ysem.at[kind, d], yrem.at[kind, d], dp, x * n_y + to)

    def start_x(kind):
        for d in (*range(1, n_x), 0):
            on_x(kind, d, lax.rem(x + d, n_x), x).start()

    def arrived_x(kind):
        on_x(kind, 0, x, x).wait()
        for d in range(1, n_x):
            on_x(kind, d, x, lax.rem(x + n_x - d, n_x)).wait_recv()

    def start_y(kind):
        for d in range(1, n_y):
            on_y(kind, d, lax.rem(y + d, n_y), y).start()

    def idx_copy(d, to, frm):
        return send(index, index_o.at[frm], isem.at[d], irem.at[d], dp, to)

    def hf_copy(i, to, frm):
        return send(
            h.at[:, pl.ds(window(to, share), win)], hf_o.at[frm], hssem.at[i], hrsem.at[i], to, me
        )

    def hf_pairs():
        for d in range(n_z):
            for c in range(2):
                if (d or c) and not far(d, n_z):
                    flip = (core + c) % 2
                    yield (
                        d * 2 + c,
                        lax.rem(z + d, n_z) * 2 + flip,
                        lax.rem(z + n_z - d, n_z) * 2 + flip,
                    )

    start_x(0)
    start_x(1)

    @pl.loop(1, n_ctx)
    def _(d):
        idx_copy(d, lax.rem(me + d, n_ctx), me).start()

    own_idx = pltpu.make_async_copy(index, index_o.at[me], lsem.at[6])
    own_idx.start()
    for i, to, frm in hf_pairs():
        hf_copy(i, to, dp).start()
    load_h.wait()
    own_hf = pltpu.make_async_copy(
        h_v.at[:, pl.ds(window(dp, share), win)], hf_o.at[dp], lsem.at[7]
    )
    own_hf.start()
    load_w.wait()
    v_v[...] = dot(h_v[...], w_v[...]).astype(BF16)
    start_x(2)
    start_x(3)
    arrived_x(0)
    start_y(0)
    arrived_x(2)
    start_y(1)
    own_idx.wait()
    own_hf.wait()
    arrived_x(1)
    arrived_x(3)
    for kind in range(2):
        for d in range(1, n_y):
            on_y(kind, d, y, lax.rem(y + n_y - d, n_y)).wait_recv()
            on_y(kind, d, lax.rem(y + d, n_y), y).wait_send()
    for kind in range(4):
        for d in range(1, n_x):
            on_x(kind, d, lax.rem(x + d, n_x), x).wait_send()

    @pl.loop(1, n_ctx)
    def _(d):
        idx_copy(d, lax.rem(me + d, n_ctx), me).wait_send()
        idx_copy(d, me, lax.rem(me + n_ctx - d, n_ctx)).wait_recv()

    for i, to, frm in hf_pairs():
        hf_copy(i, to, dp).wait_send()
        hf_copy(i, dp, frm).wait_recv()


def attend_kernel(
    sizes, q_ref, g_ref, k_ref, v_ref, dest_ref, ids_ref, qg_ref, kg_ref, fr_ref, clo_ref, slo_ref,
    gq_ref, gk_ref, gv_ref, ga_ref,
    qs, gs, kn, vs, cs, sn, c0t, s0t, es, ds_, gk_acc, gv_acc, gq_acc,
):
    n_x, n_y, rows, heads, head, n_docs = sizes
    slab = n_x * n_y * rows
    blocks = slab // rows
    tiles = slab // TILE
    factor = head ** (-0.5)
    half = head // 2
    y = lax.axis_index("ctx") % n_y

    ids = ids_ref[...]
    bounds = [jnp.sum((ids < d).astype(F32)).astype(I32) for d in range(1, n_docs)]

    def start_of(row):
        start = jnp.zeros_like(row)
        for b in bounds:
            start = jnp.where(row >= b, b, start)
        return start

    q_gain, k_gain = qg_ref[...], kg_ref[...]
    lane = lax.broadcasted_iota(I32, (1, head), 1)
    sign = jnp.where(lane < half, -1.0, 1.0).astype(F32)

    def normrope(u, gain, c, s):
        inv = lax.rsqrt(jnp.mean(u * u, axis=-1, keepdims=True) + epsilon)
        v = u * inv * gain
        return v * c + pltpu.roll(v, half, 1) * s

    def normrope_back(u, gz, gain, c, s):
        inv = lax.rsqrt(jnp.mean(u * u, axis=-1, keepdims=True) + epsilon)
        hat = u * inv
        gn = (gz * c - pltpu.roll(gz, half, 1) * s) * gain
        return inv * (gn - hat * jnp.mean(gn * hat, axis=-1, keepdims=True))

    line = lax.broadcasted_iota(I32, (blocks * n_docs, 1), 0)
    doc = line % n_docs
    first = jnp.zeros_like(line)
    for d, b in enumerate(bounds):
        first = jnp.where(doc == d + 1, b, first)
    angle = ((line // n_docs) * rows - first).astype(F32) * fr_ref[:1]
    c0t[...] = jnp.cos(angle)
    s0t[...] = jnp.sin(angle)

    def block(i):
        return pl.ds(pl.multiple_of(i * rows, rows), rows)

    @pl.loop(0, blocks)
    def _(i):
        at = block(i)
        row = lax.broadcasted_iota(I32, (rows, 1), 0) + i * rows
        c0 = jnp.broadcast_to(c0t[pl.ds(i * n_docs, 1), :], (rows, head))
        s0 = jnp.broadcast_to(s0t[pl.ds(i * n_docs, 1), :], (rows, head))
        for d, b in enumerate(bounds):
            c0 = jnp.where(row >= b, c0t[pl.ds(i * n_docs + d + 1, 1), :], c0)
            s0 = jnp.where(row >= b, s0t[pl.ds(i * n_docs + d + 1, 1), :], s0)
        clo, slo = clo_ref[...], slo_ref[...]
        c = clo * c0 - slo * s0
        s = (slo * c0 + clo * s0) * sign
        cs[at, :] = c
        sn[at, :] = s
        kn[at, :] = normrope(k_ref[i % n_y, i // n_y].astype(F32), k_gain, c, s).astype(BF16)
        gk_acc[at, :] = jnp.zeros((rows, head), F32)
        gv_acc[at, :] = jnp.zeros((rows, head), F32)

    @pl.loop(0, n_x)
    def _(m):
        at = block(m * n_y + y)
        c, s = cs[at, :], sn[at, :]
        for hd in range(heads):
            lanes = slice(hd * head, (hd + 1) * head)
            to = slice(hd * rows, (hd + 1) * rows)
            u = q_ref[m, :, lanes].astype(F32)
            qs[m, to, :] = normrope(u, q_gain, c, s).astype(BF16)
            gs[m, to, :] = g_ref[m, :, lanes]

    values = v_ref[...].reshape(slab, head)

    @pl.loop(0, tiles)
    def _(i):
        at = pl.ds(pl.multiple_of(i * TILE, TILE), TILE)
        row = lax.broadcasted_iota(I32, (TILE, 1), 0) + i * TILE
        placing = jnp.where(row == dest_ref[...], 1.0, 0.0).astype(BF16)
        vs[at, :] = dot(placing, values).astype(BF16)

    scale = factor * math.log2(math.e)
    part = heads * rows // 2

    @pl.loop(0, n_x)
    def _(m):
        i = m * n_y + y
        r0 = pl.multiple_of(i * rows, rows)
        row = lax.broadcasted_iota(I32, (1, rows), 1) + r0
        start = start_of(row)
        first = jnp.zeros((), I32)
        for b in bounds:
            first = jnp.where(r0 >= b, b, first)
        low, high = first // TILE, (r0 + rows - 1) // TILE + 1

        def forward(j, carry):
            k0 = pl.multiple_of(j * TILE, TILE)
            at = pl.ds(k0, TILE)
            key = lax.broadcasted_iota(I32, (TILE, 1), 0) + k0
            allowed = (key >= start) & (key <= row)
            sums = []
            for n in range(2):
                here = slice(n * part, (n + 1) * part)
                logits = dot(kn[at, :], qs[m, here, :], NT) * scale
                pg = dot(vs[at, :], gs[m, here, :], NT)
                e = jnp.concatenate(
                    [
                        jnp.where(allowed, jnp.exp2(logits[:, c : c + rows]), 0.0)
                        for c in range(0, part, rows)
                    ],
                    axis=1,
                )
                es[j, :, here] = e
                ds_[j, :, here] = pg
                sums.append(carry[2 * n] + jnp.sum(e, axis=0, keepdims=True))
                sums.append(carry[2 * n + 1] + jnp.sum(e * pg, axis=0, keepdims=True))
            return tuple(sums)

        zero = jnp.zeros((1, part), F32)
        sums = lax.fori_loop(low, high, forward, (zero,) * 4)
        inv = [1.0 / sums[0], 1.0 / sums[2]]
        delta = [sums[1] * inv[0], sums[3] * inv[1]]
        gq_acc[...] = jnp.zeros_like(gq_acc)

        @pl.loop(low, high)
        def _(j):
            at = pl.ds(pl.multiple_of(j * TILE, TILE), TILE)
            for n in range(2):
                here = slice(n * part, (n + 1) * part)
                p = es[j, :, here] * inv[n]
                dsj = (p * (ds_[j, :, here] - delta[n])).astype(BF16)
                gk_acc[at, :] += dot(dsj, qs[m, here, :])
                gv_acc[at, :] += dot(p.astype(BF16), gs[m, here, :])
                gq_acc[here, :] += dot(dsj, kn[at, :], TN)

        at = block(i)
        for hd in range(heads):
            lanes = slice(hd * head, (hd + 1) * head)
            gz = gq_acc[hd * rows : (hd + 1) * rows] * factor
            u = q_ref[m, :, lanes].astype(F32)
            gq_ref[m, :, lanes] = normrope_back(u, gz, q_gain, cs[at, :], sn[at, :]).astype(BF16)

    @pl.loop(0, blocks)
    def _(i):
        at = block(i)
        gz = gk_acc[at, :] * factor
        u = k_ref[i % n_y, i // n_y].astype(F32)
        gk_ref[i % n_y, i // n_y] = normrope_back(u, gz, k_gain, cs[at, :], sn[at, :]).astype(BF16)
        gv = gv_acc[at, :].astype(BF16)
        gv_ref[i % n_y, i // n_y] = gv
        vs[at, :] = gv

    @pl.loop(0, blocks)
    def _(i):
        dest = dest_ref[:, block(i)].astype(F32)
        dest = jnp.broadcast_to(dest, (rows, rows)).T
        slot = lax.broadcasted_iota(I32, (1, rows), 1).astype(F32)
        picking = jnp.concatenate(
            [
                jnp.where(dest == slot + float(c * rows), 1.0, 0.0).astype(BF16)
                for c in range(blocks)
            ],
            axis=1,
        )
        ga_ref[i // n_x, i % n_x] = dot(picking, vs[...]).astype(BF16)


def return_kernel(
    sizes, gq, gk, gv, ga, w, h, hf, gq_o, gk_o, h_o, w_o,
    r1, s1, r2, vg, ag, w_v, hf_v, hft, dw, dws, dwr,
    qsem, qrem, ysem, yrem, xsem, xrem, lsem, ag_s, ag_r, ws, wr, hssem, hrsem,
):
    n_dp, n_x, n_y, rows, width, head, share, win = sizes
    n_ctx, n_z = n_x * n_y, n_dp // 2
    dp, me = lax.axis_index("dp"), lax.axis_index("ctx")
    x, y, z, core = me // n_y, me % n_y, dp // 2, dp % 2
    after = lax.rem(z + 1, n_z) * 2 + core
    before = lax.rem(z + n_z - 1, n_z) * 2 + core
    twin = z * 2 + 1 - core
    ahead = n_z // 2
    behind = n_z - 1 - ahead

    load_w = pltpu.make_async_copy(w, w_v, lsem.at[0])
    load_w.start()

    def hf_pairs(away):
        for d in range(n_z):
            for c in range(2):
                if far(d, n_z) == away:
                    flip = (core + c) % 2
                    yield (
                        d * 2 + c,
                        lax.rem(z + d, n_z) * 2 + flip,
                        lax.rem(z + n_z - d, n_z) * 2 + flip,
                    )

    hf_loads = [
        pltpu.make_async_copy(hf.at[frm], hf_v.at[frm], hrsem.at[i])
        for i, _, frm in hf_pairs(False)
    ]
    for copy in hf_loads:
        copy.start()

    barrier = pltpu.get_barrier_semaphore()

    @pl.loop(1, n_ctx)
    def _(d):
        signal(barrier, dp, lax.rem(me + d, n_ctx))

    @pl.loop(1, n_dp)
    def _(d):
        signal(barrier, lax.rem(dp + d, n_dp), me)

    pl.semaphore_wait(barrier, n_ctx - 1 + n_dp - 1)

    grads = (ga, gv, gk)

    def on_y(kind, d, to, frm):
        src, dst = grads[kind].at[to], r1.at[kind, frm]
        if d == 0:
            return pltpu.make_async_copy(src, dst, lsem.at[1 + kind])
        return send(src, dst, ysem.at[kind, d], yrem.at[kind, d], dp, x * n_y + to)

    def on_x(kind, d, to, frm):
        dst = ag.at[dp, frm] if kind == 0 else r2.at[kind - 1, frm]
        return send(s1.at[kind, to], dst, xsem.at[kind, d], xrem.at[kind, d], dp, to * n_y + y)

    def q_copy(n, d, to, frm):
        part = width // 2
        src = gq.at[to, :, pl.ds(n * part, part)]
        dst = gq_o.at[:, pl.ds(pl.multiple_of(frm * width + n * part, part), part)]
        if d == 0:
            return pltpu.make_async_copy(src, dst, lsem.at[4 + n])
        return send(src, dst, qsem.at[n, d], qrem.at[n, d], dp, to * n_y + y)

    def hf_copy(i, to, frm):
        return send(
            h.at[:, pl.ds(window(to, share), win)], hf_v.at[frm], hssem.at[i], hrsem.at[i], to, me
        )

    def start_y(kind):
        for d in (*range(1, n_y), 0):
            on_y(kind, d, lax.rem(y + d, n_y), y).start()

    def start_q(n):
        for d in (*range(1, n_x), 0):
            q_copy(n, d, lax.rem(x + d, n_x), x).start()

    def reduce_y(kind):
        on_y(kind, 0, y, y).wait()
        for d in range(1, n_y):
            on_y(kind, d, y, lax.rem(y + n_y - d, n_y)).wait_recv()
        for m in range(n_x):
            total = r1[kind, 0, m].astype(F32)
            for f in range(1, n_y):
                total = total + r1[kind, f, m].astype(F32)
            s1[kind, m] = total.astype(BF16)

    def start_x(kind):
        for d in range(1, n_x):
            on_x(kind, d, lax.rem(x + d, n_x), x).start()

    def arrived_x(kind):
        for d in range(1, n_x):
            on_x(kind, d, x, lax.rem(x + n_x - d, n_x)).wait_recv()

    start_y(0)
    start_q(0)
    for i, to, frm in hf_pairs(True):
        hf_copy(i, to, dp).start()
    start_y(1)
    start_y(2)

    reduce_y(0)
    start_x(0)
    start_q(1)
    ag[dp, x] = s1[0, x]
    for copy in hf_loads:
        copy.wait()
    for i, _, frm in hf_pairs(False):
        hft[frm] = hf_v[frm].T
    arrived_x(0)
    chunk = n_x // 2

    def piece(slot, ch):
        return ag.at[slot, pl.ds(ch * chunk, chunk)]

    def ring(slot, ch, way, to):
        return send(piece(slot, ch), piece(slot, ch), ag_s.at[slot, way, ch], ag_r.at[slot, ch], to, me)

    sent = []

    def go(slot, ch, way, to):
        copy = ring(slot, ch, way, to)
        copy.start()
        sent.append(copy)

    for ch in range(2):
        if ahead:
            go(dp, ch, 0, after)
        if behind:
            go(dp, ch, 1, before)
    for ch in range(2):
        go(dp, ch, 2, twin)

    reduce_y(1)
    start_x(1)
    reduce_y(2)
    start_x(2)
    load_w.wait()
    r2[0, x] = s1[1, x]
    r2[1, x] = s1[2, x]
    arrived_x(1)
    for hd in range(n_x):
        vg[:, hd * head : (hd + 1) * head] = r2[0, hd]

    model = h_o.shape[1]
    steps = max(ahead, 1)
    span = model // steps
    sub = 256 if span % 256 == 0 else span
    for t in range(1, steps + 1):

        @pl.loop(0, span // sub)
        def _(n, t=t):
            at = pl.ds(pl.multiple_of((t - 1) * span + n * sub, sub), sub)
            h_o[:, at] = dot(vg[...], w_v[at, :], NT).astype(BF16)

        for ch in range(2):
            if t <= ahead:
                slot = lax.rem(z + n_z - t, n_z) * 2 + core
                ring(slot, ch, 0, after).wait_recv()
                if t < ahead:
                    go(slot, ch, 0, after)
                go(slot, ch, 2, twin)
            if t <= behind:
                slot = lax.rem(z + t, n_z) * 2 + core
                ring(slot, ch, 1, before).wait_recv()
                if t < behind:
                    go(slot, ch, 1, before)
                go(slot, ch, 2, twin)
        if t == 1:
            arrived_x(2)
            for hd in range(n_x):
                gk_o[:, hd * head : (hd + 1) * head] = r2[1, hd]
        if t == 2 or t == steps:
            if t == min(2, steps):
                for i, _, frm in hf_pairs(True):
                    hf_copy(i, dp, frm).wait_recv()
                    hft[frm] = hf_v[frm].T

    for t in range(n_z):
        slot = lax.rem(z + t, n_z) * 2 + 1 - core
        for ch in range(2):
            ring(slot, ch, 2, twin).wait_recv()

    group = 4
    for n in range(n_dp // group):
        at = slice(n * group, (n + 1) * group)
        a = jnp.concatenate([hft[e] for e in range(n * group, (n + 1) * group)], axis=1)
        b = jnp.concatenate([ag[at, hd].reshape(group * rows, head) for hd in range(n_x)], axis=1)
        if n == 0:
            dw[...] = dot(a, b)
        else:
            dw[...] += dot(a, b)
    off = pl.multiple_of(dp * share - (dp * share) // 128 * 128, 64)
    out_rows = share // n_ctx
    pad = dws.shape[1]
    for c in range(n_ctx):
        dws[c, :out_rows, :] = dw[pl.ds(off, share), :][c * out_rows : (c + 1) * out_rows].astype(BF16)
        if pad > out_rows:
            dws[c, out_rows:, :] = jnp.zeros((pad - out_rows, n_x * head), BF16)

    def w_copy(d, to, frm):
        return send(dws.at[to], dwr.at[frm], ws.at[d], wr.at[d], dp, to)

    @pl.loop(1, n_ctx)
    def _(d):
        w_copy(d, lax.rem(me + d, n_ctx), me).start()

    dwr[me] = dws[me]
    for n in range(2):
        q_copy(n, 0, x, x).wait()
        for d in range(1, n_x):
            q_copy(n, d, x, lax.rem(x + n_x - d, n_x)).wait_recv()
            q_copy(n, d, lax.rem(x + d, n_x), x).wait_send()
    for copy in sent:
        copy.wait_send()
    for kind in range(3):
        for d in range(1, n_y):
            on_y(kind, d, lax.rem(y + d, n_y), y).wait_send()
        for d in range(1, n_x):
            on_x(kind, d, lax.rem(x + d, n_x), x).wait_send()
    for i, to, _ in hf_pairs(True):
        hf_copy(i, to, dp).wait_send()

    @pl.loop(1, n_ctx)
    def _(d):
        w_copy(d, me, lax.rem(me + n_ctx - d, n_ctx)).wait_recv()

    total = dwr[0].astype(F32)
    for c in range(1, n_ctx):
        total = total + dwr[c].astype(F32)
    w_o[...] = total[:out_rows] * (1.0 / (n_dp * n_ctx))

    @pl.loop(1, n_ctx)
    def _(d):
        w_copy(d, lax.rem(me + d, n_ctx), me).wait_send()


def on_device(hidden, queries, key_states, out_grad, w_value, q_gain, k_gain, dest_rows, doc_ids):
    n_dp, n_ctx = lax.axis_size("dp"), lax.axis_size("ctx")
    rows, model = hidden.shape[1:]
    head = q_gain.shape[0]
    kv_width = key_states.shape[2]
    n_x = kv_width // head
    n_y = n_ctx // n_x
    width = queries.shape[2] // n_x
    heads = width // head
    slab = rows * n_ctx
    share = model // n_dp
    win = (share + 127) // 128 * 128
    sizes = (n_dp, n_x, n_y, rows, width, head, share, win)
    sds = jax.ShapeDtypeStruct
    dma = pltpu.SemaphoreType.DMA

    index = jnp.concatenate([dest_rows, doc_ids], axis=0)
    wide = sds((n_x, rows, width), BF16)
    narrow = sds((n_y, n_x, rows, head), BF16)
    q_in, g_in, k_in, v_in, index_in, hf = pl.pallas_call(
        functools.partial(arrive_kernel, sizes),
        out_shape=(
            wide,
            wide,
            narrow,
            narrow,
            sds((n_ctx, 2, rows), I32),
            sds((n_dp, rows, win), BF16),
        ),
        in_specs=[HBM] * 5 + [ANY],
        out_specs=(ANY,) * 6,
        scratch_shapes=[
            pltpu.VMEM((rows, model), BF16),
            pltpu.VMEM((model, kv_width), BF16),
            pltpu.VMEM((rows, kv_width), BF16),
            dma((4, n_x)),
            dma((4, n_x)),
            dma((2, n_y)),
            dma((2, n_y)),
            dma((n_ctx,)),
            dma((n_ctx,)),
            dma((n_dp,)),
            dma((n_dp,)),
            dma((8,)),
        ],
        compiler_params=pltpu.CompilerParams(
            collective_id=0, has_side_effects=True, vmem_limit_bytes=16 << 20
        ),
        name="arrive",
    )(*[pltpu.with_memory_space_constraint(a, pltpu.HBM) for a in (queries[0], out_grad[0], key_states[0], hidden[0], w_value)], index)

    dest_all = index_in[:, 0].reshape(n_x, n_y, rows).transpose(1, 0, 2).reshape(1, slab)
    ids_all = index_in[:, 1]
    half = head // 2
    frequency = rope_base ** (-(np.arange(half, dtype=np.float64) * 2.0 / head))
    frequency = np.concatenate([frequency, frequency])[None]
    low = np.arange(rows, dtype=np.float64)[:, None] * frequency
    consts = [
        jnp.asarray(np.broadcast_to(frequency, (8, head)), F32),
        jnp.asarray(np.cos(low), F32),
        jnp.asarray(np.sin(low), F32),
    ]
    tiles = slab // TILE
    n_docs = 4
    gq, gk, gv, ga = pl.pallas_call(
        functools.partial(attend_kernel, (n_x, n_y, rows, heads, head, n_docs)),
        out_shape=(wide, narrow, narrow, narrow),
        in_specs=[VMEM] * 11,
        out_specs=(VMEM,) * 4,
        scratch_shapes=[
            pltpu.VMEM((n_x, heads * rows, head), BF16),
            pltpu.VMEM((n_x, heads * rows, head), BF16),
            pltpu.VMEM((slab, head), BF16),
            pltpu.VMEM((slab, head), BF16),
            pltpu.VMEM((slab, head), F32),
            pltpu.VMEM((slab, head), F32),
            pltpu.VMEM((n_ctx * n_docs, head), F32),
            pltpu.VMEM((n_ctx * n_docs, head), F32),
            pltpu.VMEM((tiles, TILE, heads * rows), F32),
            pltpu.VMEM((tiles, TILE, heads * rows), F32),
            pltpu.VMEM((slab, head), F32),
            pltpu.VMEM((slab, head), F32),
            pltpu.VMEM((heads * rows, head), F32),
        ],
        compiler_params=pltpu.CompilerParams(vmem_limit_bytes=44 << 20),
        name="attend",
    )(q_in, g_in, k_in, v_in, dest_all, ids_all, q_gain[None], k_gain[None], *consts)

    out_rows = share // n_ctx
    pad = (out_rows + 15) // 16 * 16
    query_grad, key_grad, hidden_grad, weight_grad = pl.pallas_call(
        functools.partial(return_kernel, sizes),
        out_shape=(
            sds((rows, n_x * width), BF16),
            sds((rows, kv_width), BF16),
            sds((rows, model), BF16),
            sds((out_rows, kv_width), F32),
        ),
        in_specs=[ANY] * 4 + [HBM] * 2 + [ANY],
        out_specs=(ANY, VMEM, VMEM, VMEM),
        scratch_shapes=[
            pltpu.VMEM((3, n_y, n_x, rows, head), BF16),
            pltpu.VMEM((3, n_x, rows, head), BF16),
            pltpu.VMEM((2, n_x, rows, head), BF16),
            pltpu.VMEM((rows, kv_width), BF16),
            pltpu.VMEM((n_dp, n_x, rows, head), BF16),
            pltpu.VMEM((model, kv_width), BF16),
            pltpu.VMEM((n_dp, rows, win), BF16),
            pltpu.VMEM((n_dp, win, rows), BF16),
            pltpu.VMEM((win, kv_width), F32),
            pltpu.VMEM((n_ctx, pad, kv_width), BF16),
            pltpu.VMEM((n_ctx, pad, kv_width), BF16),
            dma((2, n_x)),
            dma((2, n_x)),
            dma((3, n_y)),
            dma((3, n_y)),
            dma((3, n_x)),
            dma((3, n_x)),
            dma((6,)),
            dma((n_dp, 3, 2)),
            dma((n_dp, 2)),
            dma((n_ctx,)),
            dma((n_ctx,)),
            dma((n_dp,)),
            dma((n_dp,)),
        ],
        compiler_params=pltpu.CompilerParams(
            collective_id=1, has_side_effects=True, vmem_limit_bytes=32 << 20
        ),
        name="give_back",
    )(gq, gk, gv, ga, w_value, hidden[0], hf)
    return (hidden_grad[None], query_grad[None], key_grad[None], weight_grad)


def solution(mesh):
    rows = P("dp", "ctx", None)
    return jax.shard_map(
        on_device,
        mesh=mesh,
        in_specs=(rows, rows, rows, rows, P(), P(), P(), P("dp", "ctx"), P("dp", "ctx")),
        out_specs=(rows, rows, rows, P(("dp", "ctx"), None)),
        check_vma=False,
    )
```

```python
import functools
import math

import jax
import jax.numpy as jnp
import numpy as np
from jax import lax
from jax.experimental import pallas as pl
from jax.experimental.pallas import tpu as pltpu
from jax.sharding import PartitionSpec as P

epsilon = 1e-06
rope_base = 1000000.0
BF16, F32, I32 = jnp.bfloat16, jnp.float32, jnp.int32
ANY = pl.BlockSpec(memory_space=pl.ANY)
HBM = pl.BlockSpec(memory_space=pltpu.HBM)
VMEM = pl.BlockSpec(memory_space=pltpu.VMEM)
TILE = 256
NT = (((1,), (1,)), ((), ()))
TN = (((0,), (0,)), ((), ()))


def dot(a, b, dims=(((1,), (0,)), ((), ()))):
    return lax.dot_general(a, b, dims, preferred_element_type=F32)


def send(src, dst, ssem, rsem, dp, ctx):
    return pltpu.make_async_remote_copy(
        src_ref=src,
        dst_ref=dst,
        send_sem=ssem,
        recv_sem=rsem,
        device_id=(dp, ctx),
        device_id_type=pl.DeviceIdType.MESH,
    )


def signal(sem, dp, ctx):
    pl.semaphore_signal(
        sem, inc=1, device_id=(dp, ctx), device_id_type=pl.DeviceIdType.MESH
    )


def window(dp, share):
    return pl.multiple_of((dp * share) // 128 * 128, 128)


def head_lanes(head):
    lane = lax.broadcasted_iota(I32, (1, head), 1)
    return jnp.where(lane < head // 2, -1.0, 1.0).astype(F32)


def normrope(u, gain, c, s):
    inv = lax.rsqrt(jnp.mean(u * u, axis=-1, keepdims=True) + epsilon)
    v = u * inv * gain
    return v * c + pltpu.roll(v, u.shape[-1] // 2, 1) * s


def normrope_back(u, gz, gain, c, s):
    inv = lax.rsqrt(jnp.mean(u * u, axis=-1, keepdims=True) + epsilon)
    hat = u * inv
    gn = (gz * c - pltpu.roll(gz, u.shape[-1] // 2, 1) * s) * gain
    return inv * (gn - hat * jnp.mean(gn * hat, axis=-1, keepdims=True))


def far(d, n_z):
    return n_z == 8 and d in (3, 5)


def arrive_kernel(
    sizes, q, g, k, h, w, index, qg_ref, kg_ref, fr_ref, clo_ref, slo_ref,
    q_o, g_o, k_o, index_o, hf_o, cs, sn, kn, qs, vs,
    h_v, w_v, v_v, v_o, c0t, s0t, ssem, rsem, ysem, yrem, isem, irem, hssem, hrsem, lsem,
):
    n_dp, n_x, n_y, rows, width, head, share, win = sizes
    n_ctx, n_z = n_x * n_y, n_dp // 2
    dp, me = lax.axis_index("dp"), lax.axis_index("ctx")
    x, y, z, core = me // n_y, me % n_y, dp // 2, dp % 2

    load_h = pltpu.make_async_copy(h, h_v, lsem.at[0])
    load_w = pltpu.make_async_copy(w, w_v, lsem.at[1])
    load_h.start()
    load_w.start()

    barrier = pltpu.get_barrier_semaphore()

    @pl.loop(1, n_ctx)
    def _(d):
        signal(barrier, dp, lax.rem(me + d, n_ctx))

    @pl.loop(1, n_dp)
    def _(d):
        signal(barrier, lax.rem(dp + d, n_dp), me)

    pl.semaphore_wait(barrier, n_ctx - 1 + n_dp - 1)

    def cols(s, size):
        return pl.ds(pl.multiple_of(s * size, size), size)

    def on_x(kind, d, to, frm):
        src, dst = (
            (k.at[:, cols(to, head)], k_o.at[y, frm]),
            (q.at[:, cols(to, width)], q_o.at[frm]),
            (v_v.at[:, cols(to, head)], v_o.at[y, frm]),
            (g.at[:, cols(to, width)], g_o.at[frm]),
        )[kind]
        if d == 0:
            return pltpu.make_async_copy(src, dst, lsem.at[2 + kind])
        return send(src, dst, ssem.at[kind, d], rsem.at[kind, d], dp, to * n_y + y)

    def on_y(kind, d, to, frm):
        ref = (k_o, v_o)[kind]
        return send(ref.at[frm], ref.at[frm], ysem.at[kind, d], yrem.at[kind, d], dp, x * n_y + to)

    def start_x(kind):
        for d in (*range(1, n_x), 0):
            on_x(kind, d, lax.rem(x + d, n_x), x).start()

    def arrived_x(kind):
        on_x(kind, 0, x, x).wait()
        for d in range(1, n_x):
            on_x(kind, d, x, lax.rem(x + n_x - d, n_x)).wait_recv()

    def start_y(kind):
        for d in range(1, n_y):
            on_y(kind, d, lax.rem(y + d, n_y), y).start()

    def idx_copy(d, to, frm):
        return send(index, index_o.at[frm], isem.at[d], irem.at[d], dp, to)

    def hf_copy(i, to, frm):
        return send(
            h.at[:, pl.ds(window(to, share), win)], hf_o.at[frm], hssem.at[i], hrsem.at[i], to, me
        )

    def hf_pairs():
        for d in range(n_z):
            for c in range(2):
                if (d or c) and not far(d, n_z):
                    flip = (core + c) % 2
                    yield (
                        d * 2 + c,
                        lax.rem(z + d, n_z) * 2 + flip,
                        lax.rem(z + n_z - d, n_z) * 2 + flip,
                    )

    start_x(0)
    start_x(1)

    @pl.loop(1, n_ctx)
    def _(d):
        idx_copy(d, lax.rem(me + d, n_ctx), me).start()

    own_idx = pltpu.make_async_copy(index, index_o.at[me], lsem.at[6])
    own_idx.start()
    for i, to, frm in hf_pairs():
        hf_copy(i, to, dp).start()
    load_h.wait()
    own_hf = pltpu.make_async_copy(
        h_v.at[:, pl.ds(window(dp, share), win)], hf_o.at[dp], lsem.at[7]
    )
    own_hf.start()
    load_w.wait()
    v_v[...] = dot(h_v[...], w_v[...]).astype(BF16)
    start_x(2)
    start_x(3)
    arrived_x(0)
    start_y(0)

    @pl.loop(1, n_ctx)
    def _(d):
        idx_copy(d, me, lax.rem(me + n_ctx - d, n_ctx)).wait_recv()

    own_idx.wait()

    n_docs = c0t.shape[0] // n_ctx
    ids = index_o[:, 1, :]
    bounds = [
        jnp.sum(jnp.sum((ids < d).astype(F32), axis=1, keepdims=True), axis=0, keepdims=True).astype(I32)
        for d in range(1, n_docs)
    ]
    line = lax.broadcasted_iota(I32, (n_ctx * n_docs, 1), 0)
    doc = line % n_docs
    first = jnp.zeros_like(line)
    for d, b in enumerate(bounds):
        first = jnp.where(doc == d + 1, b, first)
    angle = ((line // n_docs) * rows - first).astype(F32) * fr_ref[:1]
    c0t[...] = jnp.cos(angle)
    s0t[...] = jnp.sin(angle)
    sign = head_lanes(head)

    def block(i):
        return pl.ds(pl.multiple_of(i * rows, rows), rows)

    @pl.loop(0, n_ctx)
    def _(i):
        at = block(i)
        row = lax.broadcasted_iota(I32, (rows, 1), 0) + i * rows
        c0 = jnp.broadcast_to(c0t[pl.ds(i * n_docs, 1), :], (rows, head))
        s0 = jnp.broadcast_to(s0t[pl.ds(i * n_docs, 1), :], (rows, head))
        for d, b in enumerate(bounds):
            c0 = jnp.where(row >= b, c0t[pl.ds(i * n_docs + d + 1, 1), :], c0)
            s0 = jnp.where(row >= b, s0t[pl.ds(i * n_docs + d + 1, 1), :], s0)
        clo, slo = clo_ref[...], slo_ref[...]
        cs[at, :] = clo * c0 - slo * s0
        sn[at, :] = (slo * c0 + clo * s0) * sign

    arrived_x(1)

    @pl.loop(0, n_x)
    def _(m):
        at = block(m * n_y + y)
        c, s = cs[at, :], sn[at, :]
        for hd in range(width // head):
            u = q_o[m, :, hd * head : (hd + 1) * head].astype(F32)
            qs[m, hd * rows : (hd + 1) * rows, :] = normrope(u, qg_ref[...], c, s).astype(BF16)

    arrived_x(2)
    start_y(1)
    for d in range(1, n_y):
        on_y(0, d, y, lax.rem(y + n_y - d, n_y)).wait_recv()

    @pl.loop(0, n_ctx)
    def _(i):
        at = block(i)
        u = k_o[i % n_y, i // n_y].astype(F32)
        kn[at, :] = normrope(u, kg_ref[...], cs[at, :], sn[at, :]).astype(BF16)

    for d in range(1, n_y):
        on_y(1, d, y, lax.rem(y + n_y - d, n_y)).wait_recv()
    dest = jnp.concatenate(
        [index_o[m * n_y + f, :1, :] for f in range(n_y) for m in range(n_x)], axis=1
    )
    slab = n_ctx * rows

    @pl.loop(0, slab // TILE)
    def _(i):
        at = pl.ds(pl.multiple_of(i * TILE, TILE), TILE)
        row = lax.broadcasted_iota(I32, (TILE, 1), 0) + i * TILE
        placing = jnp.where(row == dest, 1.0, 0.0).astype(BF16)
        vs[at, :] = dot(placing, v_o[...].reshape(slab, head)).astype(BF16)

    own_hf.wait()
    arrived_x(3)
    for kind in range(2):
        for d in range(1, n_y):
            on_y(kind, d, lax.rem(y + d, n_y), y).wait_send()
    for kind in range(4):
        for d in range(1, n_x):
            on_x(kind, d, lax.rem(x + d, n_x), x).wait_send()

    @pl.loop(1, n_ctx)
    def _(d):
        idx_copy(d, lax.rem(me + d, n_ctx), me).wait_send()

    for i, to, frm in hf_pairs():
        hf_copy(i, to, dp).wait_send()
        hf_copy(i, dp, frm).wait_recv()


def attend_kernel(
    sizes, qs, g_ref, kn, vs, index_ref,
    gq_ref, gk_ref, gv_ref, ga_ref,
    gs, es, ds_, gv_acc, gvt,
):
    n_x, n_y, rows, heads, head, n_docs = sizes
    slab = n_x * n_y * rows
    blocks = slab // rows
    factor = head ** (-0.5)
    y = lax.axis_index("ctx") % n_y

    ids = index_ref[:, 1, :]
    bounds = [jnp.sum((ids < d).astype(F32)).astype(I32) for d in range(1, n_docs)]

    def start_of(row):
        start = jnp.zeros_like(row)
        for b in bounds:
            start = jnp.where(row >= b, b, start)
        return start

    def block(i):
        return pl.ds(pl.multiple_of(i * rows, rows), rows)

    gk_ref[...] = jnp.zeros_like(gk_ref)
    gv_acc[...] = jnp.zeros_like(gv_acc)
    for m in range(n_x):
        for hd in range(heads):
            gs[m, hd * rows : (hd + 1) * rows, :] = g_ref[m, :, hd * head : (hd + 1) * head]

    scale = factor * math.log2(math.e)
    part = heads * rows // 2

    @pl.loop(0, n_x)
    def _(m):
        i = m * n_y + y
        r0 = pl.multiple_of(i * rows, rows)
        row = lax.broadcasted_iota(I32, (1, rows), 1) + r0
        start = start_of(row)
        first = jnp.zeros((), I32)
        for b in bounds:
            first = jnp.where(r0 >= b, b, first)
        low, high = first // TILE, (r0 + rows - 1) // TILE + 1

        def forward(j, carry):
            k0 = pl.multiple_of(j * TILE, TILE)
            at = pl.ds(k0, TILE)
            key = lax.broadcasted_iota(I32, (TILE, 1), 0) + k0
            allowed = (key >= start) & (key <= row)
            sums = []
            for n in range(2):
                here = slice(n * part, (n + 1) * part)
                logits = dot(kn[at, :], qs[m, here, :], NT) * scale
                pg = dot(vs[at, :], gs[m, here, :], NT)
                e = jnp.concatenate(
                    [
                        jnp.where(allowed, jnp.exp2(logits[:, c : c + rows]), 0.0)
                        for c in range(0, part, rows)
                    ],
                    axis=1,
                )
                es[j, :, here] = e
                ds_[j, :, here] = pg
                sums.append(carry[2 * n] + jnp.sum(e, axis=0, keepdims=True))
                sums.append(carry[2 * n + 1] + jnp.sum(e * pg, axis=0, keepdims=True))
            return tuple(sums)

        zero = jnp.zeros((1, part), F32)
        sums = lax.fori_loop(low, high, forward, (zero,) * 4)
        inv = [1.0 / sums[0], 1.0 / sums[2]]
        delta = [sums[1] * inv[0], sums[3] * inv[1]]
        gq_ref[m] = jnp.zeros((heads * rows, head), F32)

        @pl.loop(low, high)
        def _(j):
            at = pl.ds(pl.multiple_of(j * TILE, TILE), TILE)
            for n in range(2):
                here = slice(n * part, (n + 1) * part)
                p = es[j, :, here] * inv[n]
                dsj = (p * (ds_[j, :, here] - delta[n])).astype(BF16)
                gk_ref[at, :] += dot(dsj, qs[m, here, :])
                gv_acc[at, :] += dot(p.astype(BF16), gs[m, here, :])
                gq_ref[m, here, :] += dot(dsj, kn[at, :], TN)

    @pl.loop(0, blocks)
    def _(i):
        gv = gv_acc[block(i), :]
        gv_ref[i % n_y, i // n_y] = gv.astype(BF16)
        gvt[:, block(i)] = gv.T.astype(BF16)

    for f in range(n_y):
        for m in range(0, n_x, 2):
            dest = jnp.concatenate(
                [index_ref[(m + n) * n_y + f, :1, :] for n in range(2)], axis=1
            )
            row = lax.broadcasted_iota(I32, (slab, 1), 0)
            picking = jnp.where(row == dest, 1.0, 0.0).astype(BF16)
            moved = dot(gvt[...], picking).T.astype(BF16)
            for n in range(2):
                ga_ref[f, m + n] = moved[n * rows : (n + 1) * rows]


def return_kernel(
    sizes, gq_raw, gk_raw, gv, ga, w, h, hf, q_in, k_in, cs, sn, qg_ref, kg_ref,
    gq_o, gk_o, h_o, w_o,
    gq, gk, r1, s1, r2, vg, ag, w_v, hf_v, hft, dw, dws, dwr,
    qsem, qrem, ysem, yrem, xsem, xrem, lsem, ag_s, ag_r, ws, wr, hssem, hrsem,
):
    n_dp, n_x, n_y, rows, width, head, share, win = sizes
    n_ctx, n_z = n_x * n_y, n_dp // 2
    dp, me = lax.axis_index("dp"), lax.axis_index("ctx")
    x, y, z, core = me // n_y, me % n_y, dp // 2, dp % 2
    after = lax.rem(z + 1, n_z) * 2 + core
    before = lax.rem(z + n_z - 1, n_z) * 2 + core
    twin = z * 2 + 1 - core
    ahead = n_z // 2
    behind = n_z - 1 - ahead

    load_w = pltpu.make_async_copy(w, w_v, lsem.at[0])
    load_w.start()

    def hf_pairs(away):
        for d in range(n_z):
            for c in range(2):
                if far(d, n_z) == away:
                    flip = (core + c) % 2
                    yield (
                        d * 2 + c,
                        lax.rem(z + d, n_z) * 2 + flip,
                        lax.rem(z + n_z - d, n_z) * 2 + flip,
                    )

    hf_loads = [
        pltpu.make_async_copy(hf.at[frm], hf_v.at[frm], hrsem.at[i])
        for i, _, frm in hf_pairs(False)
    ]
    for copy in hf_loads:
        copy.start()

    barrier = pltpu.get_barrier_semaphore()

    @pl.loop(1, n_ctx)
    def _(d):
        signal(barrier, dp, lax.rem(me + d, n_ctx))

    @pl.loop(1, n_dp)
    def _(d):
        signal(barrier, lax.rem(dp + d, n_dp), me)

    pl.semaphore_wait(barrier, n_ctx - 1 + n_dp - 1)

    grads = (ga, gv, gk)

    def on_y(kind, d, to, frm):
        src, dst = grads[kind].at[to], r1.at[kind, frm]
        if d == 0:
            return pltpu.make_async_copy(src, dst, lsem.at[1 + kind])
        return send(src, dst, ysem.at[kind, d], yrem.at[kind, d], dp, x * n_y + to)

    def on_x(kind, d, to, frm):
        dst = ag.at[dp, frm] if kind == 0 else r2.at[kind - 1, frm]
        return send(s1.at[kind, to], dst, xsem.at[kind, d], xrem.at[kind, d], dp, to * n_y + y)

    def q_copy(n, d, to, frm):
        part = width // 2
        src = gq.at[to, :, pl.ds(n * part, part)]
        dst = gq_o.at[:, pl.ds(pl.multiple_of(frm * width + n * part, part), part)]
        if d == 0:
            return pltpu.make_async_copy(src, dst, lsem.at[4 + n])
        return send(src, dst, qsem.at[n, d], qrem.at[n, d], dp, to * n_y + y)

    def hf_copy(i, to, frm):
        return send(
            h.at[:, pl.ds(window(to, share), win)], hf_v.at[frm], hssem.at[i], hrsem.at[i], to, me
        )

    def start_y(kind):
        for d in (*range(1, n_y), 0):
            on_y(kind, d, lax.rem(y + d, n_y), y).start()

    def start_q(n):
        for d in (*range(1, n_x), 0):
            q_copy(n, d, lax.rem(x + d, n_x), x).start()

    def reduce_y(kind):
        on_y(kind, 0, y, y).wait()
        for d in range(1, n_y):
            on_y(kind, d, y, lax.rem(y + n_y - d, n_y)).wait_recv()
        for m in range(n_x):
            total = r1[kind, 0, m].astype(F32)
            for f in range(1, n_y):
                total = total + r1[kind, f, m].astype(F32)
            s1[kind, m] = total.astype(BF16)

    def start_x(kind):
        for d in range(1, n_x):
            on_x(kind, d, lax.rem(x + d, n_x), x).start()

    def arrived_x(kind):
        for d in range(1, n_x):
            on_x(kind, d, x, lax.rem(x + n_x - d, n_x)).wait_recv()

    start_y(0)
    for i, to, frm in hf_pairs(True):
        hf_copy(i, to, dp).start()
    factor = head ** (-0.5)

    @pl.loop(0, n_x)
    def _(m):
        at = pl.ds(pl.multiple_of((m * n_y + y) * rows, rows), rows)
        c, s = cs[at, :], sn[at, :]
        for hd in range(width // head):
            lanes = slice(hd * head, (hd + 1) * head)
            gz = gq_raw[m, hd * rows : (hd + 1) * rows, :] * factor
            u = q_in[m, :, lanes].astype(F32)
            gq[m, :, lanes] = normrope_back(u, gz, qg_ref[...], c, s).astype(BF16)

    start_q(0)
    start_y(1)

    @pl.loop(0, n_ctx)
    def _(i):
        at = pl.ds(pl.multiple_of(i * rows, rows), rows)
        gz = gk_raw[at, :] * factor
        u = k_in[i % n_y, i // n_y].astype(F32)
        gk[i % n_y, i // n_y] = normrope_back(u, gz, kg_ref[...], cs[at, :], sn[at, :]).astype(BF16)

    reduce_y(0)
    start_x(0)
    start_y(2)
    start_q(1)
    ag[dp, x] = s1[0, x]
    for copy in hf_loads:
        copy.wait()
    for i, _, frm in hf_pairs(False):
        hft[frm] = hf_v[frm].T
    arrived_x(0)

    def piece(slot, ch):
        return ag.at[slot, ch]

    def takes(t, ch, way):
        return t <= behind or (t == ahead and (ch < n_x // 2) == (way == 0))

    def ring(slot, ch, way, to):
        return send(piece(slot, ch), piece(slot, ch), ag_s.at[slot, way, ch], ag_r.at[slot, ch], to, me)

    sent = []

    def go(slot, ch, way, to):
        copy = ring(slot, ch, way, to)
        copy.start()
        sent.append(copy)

    for ch in range(n_x):
        if takes(1, ch, 0):
            go(dp, ch, 0, after)
        if takes(1, ch, 1):
            go(dp, ch, 1, before)
    for ch in range(n_x):
        go(dp, ch, 2, twin)

    reduce_y(1)
    start_x(1)
    reduce_y(2)
    start_x(2)
    load_w.wait()
    r2[0, x] = s1[1, x]
    r2[1, x] = s1[2, x]
    arrived_x(1)
    for hd in range(n_x):
        vg[:, hd * head : (hd + 1) * head] = r2[0, hd]

    model = h_o.shape[1]
    steps = max(ahead, 1)
    span = model // steps
    sub = 256 if span % 256 == 0 else span
    for t in range(1, steps + 1):

        @pl.loop(0, span // sub)
        def _(n, t=t):
            at = pl.ds(pl.multiple_of((t - 1) * span + n * sub, sub), sub)
            h_o[:, at] = dot(vg[...], w_v[at, :], NT).astype(BF16)

        for ch in range(n_x):
            for way, to, hop in ((0, after, n_z - t), (1, before, t)):
                if takes(t, ch, way):
                    slot = lax.rem(z + hop, n_z) * 2 + core
                    ring(slot, ch, way, to).wait_recv()
                    if takes(t + 1, ch, way):
                        go(slot, ch, way, to)
                    go(slot, ch, 2, twin)
        if t == 1:
            arrived_x(2)
            for hd in range(n_x):
                gk_o[:, hd * head : (hd + 1) * head] = r2[1, hd]
        if t == 2 or t == steps:
            if t == min(2, steps):
                for i, _, frm in hf_pairs(True):
                    hf_copy(i, dp, frm).wait_recv()
                    hft[frm] = hf_v[frm].T

    for t in range(n_z):
        slot = lax.rem(z + t, n_z) * 2 + 1 - core
        for ch in range(n_x):
            ring(slot, ch, 2, twin).wait_recv()

    group = 4
    for n in range(n_dp // group):
        at = slice(n * group, (n + 1) * group)
        a = jnp.concatenate([hft[e] for e in range(n * group, (n + 1) * group)], axis=1)
        b = jnp.concatenate([ag[at, hd].reshape(group * rows, head) for hd in range(n_x)], axis=1)
        if n == 0:
            dw[...] = dot(a, b)
        else:
            dw[...] += dot(a, b)
    off = pl.multiple_of(dp * share - (dp * share) // 128 * 128, 64)
    out_rows = share // n_ctx
    pad = dws.shape[1]
    for c in range(n_ctx):
        dws[c, :out_rows, :] = dw[pl.ds(off, share), :][c * out_rows : (c + 1) * out_rows].astype(BF16)
        if pad > out_rows:
            dws[c, out_rows:, :] = jnp.zeros((pad - out_rows, n_x * head), BF16)

    def w_copy(d, to, frm):
        return send(dws.at[to], dwr.at[frm], ws.at[d], wr.at[d], dp, to)

    @pl.loop(1, n_ctx)
    def _(d):
        w_copy(d, lax.rem(me + d, n_ctx), me).start()

    dwr[me] = dws[me]
    for n in range(2):
        q_copy(n, 0, x, x).wait()
        for d in range(1, n_x):
            q_copy(n, d, x, lax.rem(x + n_x - d, n_x)).wait_recv()
            q_copy(n, d, lax.rem(x + d, n_x), x).wait_send()
    for copy in sent:
        copy.wait_send()
    for kind in range(3):
        for d in range(1, n_y):
            on_y(kind, d, lax.rem(y + d, n_y), y).wait_send()
        for d in range(1, n_x):
            on_x(kind, d, lax.rem(x + d, n_x), x).wait_send()
    for i, to, _ in hf_pairs(True):
        hf_copy(i, to, dp).wait_send()

    @pl.loop(1, n_ctx)
    def _(d):
        w_copy(d, me, lax.rem(me + n_ctx - d, n_ctx)).wait_recv()

    total = dwr[0].astype(F32)
    for c in range(1, n_ctx):
        total = total + dwr[c].astype(F32)
    w_o[...] = total[:out_rows] * (1.0 / (n_dp * n_ctx))

    @pl.loop(1, n_ctx)
    def _(d):
        w_copy(d, lax.rem(me + d, n_ctx), me).wait_send()


def on_device(hidden, queries, key_states, out_grad, w_value, q_gain, k_gain, dest_rows, doc_ids):
    n_dp, n_ctx = lax.axis_size("dp"), lax.axis_size("ctx")
    rows, model = hidden.shape[1:]
    head = q_gain.shape[0]
    kv_width = key_states.shape[2]
    n_x = kv_width // head
    n_y = n_ctx // n_x
    width = queries.shape[2] // n_x
    heads = width // head
    slab = rows * n_ctx
    share = model // n_dp
    win = (share + 127) // 128 * 128
    sizes = (n_dp, n_x, n_y, rows, width, head, share, win)
    sds = jax.ShapeDtypeStruct
    dma = pltpu.SemaphoreType.DMA

    index = jnp.concatenate([dest_rows, doc_ids], axis=0)
    wide = sds((n_x, rows, width), BF16)
    narrow = sds((n_y, n_x, rows, head), BF16)
    half = head // 2
    frequency = rope_base ** (-(np.arange(half, dtype=np.float64) * 2.0 / head))
    frequency = np.concatenate([frequency, frequency])[None]
    low = np.arange(rows, dtype=np.float64)[:, None] * frequency
    consts = [
        jnp.asarray(np.broadcast_to(frequency, (8, head)), F32),
        jnp.asarray(np.cos(low), F32),
        jnp.asarray(np.sin(low), F32),
    ]
    n_docs = 4
    stacked = (n_x, heads * rows, head)
    flat = sds((slab, head), BF16)
    kept = [
        pltpu.with_memory_space_constraint(a, pltpu.HBM)
        for a in (queries[0], out_grad[0], key_states[0], hidden[0], w_value)
    ]
    q_in, g_in, k_in, index_in, hf, cs, sn, kn, qs, vs = pl.pallas_call(
        functools.partial(arrive_kernel, sizes),
        out_shape=(
            wide,
            wide,
            narrow,
            sds((n_ctx, 2, rows), I32),
            sds((n_dp, rows, win), BF16),
            sds((slab, head), F32),
            sds((slab, head), F32),
            flat,
            sds(stacked, BF16),
            flat,
        ),
        in_specs=[HBM] * 5 + [ANY] + [VMEM] * 5,
        out_specs=(VMEM, ANY, VMEM, VMEM, ANY) + (VMEM,) * 5,
        scratch_shapes=[
            pltpu.VMEM((rows, model), BF16),
            pltpu.VMEM((model, kv_width), BF16),
            pltpu.VMEM((rows, kv_width), BF16),
            pltpu.VMEM((n_y, n_x, rows, head), BF16),
            pltpu.VMEM((n_ctx * n_docs, head), F32),
            pltpu.VMEM((n_ctx * n_docs, head), F32),
            dma((4, n_x)),
            dma((4, n_x)),
            dma((2, n_y)),
            dma((2, n_y)),
            dma((n_ctx,)),
            dma((n_ctx,)),
            dma((n_dp,)),
            dma((n_dp,)),
            dma((8,)),
        ],
        compiler_params=pltpu.CompilerParams(
            collective_id=0, has_side_effects=True, vmem_limit_bytes=24 << 20
        ),
        name="arrive",
    )(*kept, index, q_gain[None], k_gain[None], *consts)

    tiles = slab // TILE
    gq, gk, gv, ga = pl.pallas_call(
        functools.partial(attend_kernel, (n_x, n_y, rows, heads, head, n_docs)),
        out_shape=(sds(stacked, F32), sds((slab, head), F32), narrow, narrow),
        in_specs=[VMEM] * 5,
        out_specs=(VMEM,) * 4,
        scratch_shapes=[
            pltpu.VMEM(stacked, BF16),
            pltpu.VMEM((tiles, TILE, heads * rows), F32),
            pltpu.VMEM((tiles, TILE, heads * rows), F32),
            pltpu.VMEM((slab, head), F32),
            pltpu.VMEM((head, slab), BF16),
        ],
        compiler_params=pltpu.CompilerParams(vmem_limit_bytes=36 << 20),
        name="attend",
    )(qs, g_in, kn, vs, index_in)

    out_rows = share // n_ctx
    pad = (out_rows + 15) // 16 * 16
    query_grad, key_grad, hidden_grad, weight_grad = pl.pallas_call(
        functools.partial(return_kernel, sizes),
        out_shape=(
            sds((rows, n_x * width), BF16),
            sds((rows, kv_width), BF16),
            sds((rows, model), BF16),
            sds((out_rows, kv_width), F32),
        ),
        in_specs=[VMEM] * 2 + [ANY] * 2 + [HBM] * 2 + [ANY] + [VMEM] * 6,
        out_specs=(ANY, VMEM, VMEM, VMEM),
        scratch_shapes=[
            pltpu.VMEM((n_x, rows, width), BF16),
            pltpu.VMEM((n_y, n_x, rows, head), BF16),
            pltpu.VMEM((3, n_y, n_x, rows, head), BF16),
            pltpu.VMEM((3, n_x, rows, head), BF16),
            pltpu.VMEM((2, n_x, rows, head), BF16),
            pltpu.VMEM((rows, kv_width), BF16),
            pltpu.VMEM((n_dp, n_x, rows, head), BF16),
            pltpu.VMEM((model, kv_width), BF16),
            pltpu.VMEM((n_dp, rows, win), BF16),
            pltpu.VMEM((n_dp, win, rows), BF16),
            pltpu.VMEM((win, kv_width), F32),
            pltpu.VMEM((n_ctx, pad, kv_width), BF16),
            pltpu.VMEM((n_ctx, pad, kv_width), BF16),
            dma((2, n_x)),
            dma((2, n_x)),
            dma((3, n_y)),
            dma((3, n_y)),
            dma((3, n_x)),
            dma((3, n_x)),
            dma((6,)),
            dma((n_dp, 3, n_x)),
            dma((n_dp, n_x)),
            dma((n_ctx,)),
            dma((n_ctx,)),
            dma((n_dp,)),
            dma((n_dp,)),
        ],
        compiler_params=pltpu.CompilerParams(
            collective_id=1, has_side_effects=True, vmem_limit_bytes=32 << 20
        ),
        name="give_back",
    )(gq, gk, gv, ga, w_value, hidden[0], hf, q_in, k_in, cs, sn, q_gain[None], k_gain[None])
    return (hidden_grad[None], query_grad[None], key_grad[None], weight_grad)


def solution(mesh):
    rows = P("dp", "ctx", None)
    return jax.shard_map(
        on_device,
        mesh=mesh,
        in_specs=(rows, rows, rows, rows, P(), P(), P(), P("dp", "ctx"), P("dp", "ctx")),
        out_specs=(rows, rows, rows, P(("dp", "ctx"), None)),
        check_vma=False,
    )
```

```python
import functools
import math

import jax
import jax.numpy as jnp
import numpy as np
from jax import lax
from jax.experimental import pallas as pl
from jax.experimental.pallas import tpu as pltpu
from jax.sharding import PartitionSpec as P

epsilon = 1e-06
rope_base = 1000000.0
BF16, F32, I32 = jnp.bfloat16, jnp.float32, jnp.int32
ANY = pl.BlockSpec(memory_space=pl.ANY)
HBM = pl.BlockSpec(memory_space=pltpu.HBM)
VMEM = pl.BlockSpec(memory_space=pltpu.VMEM)
TILE = 256
NT = (((1,), (1,)), ((), ()))
TN = (((0,), (0,)), ((), ()))


def dot(a, b, dims=(((1,), (0,)), ((), ()))):
    return lax.dot_general(a, b, dims, preferred_element_type=F32)


def send(src, dst, ssem, rsem, dp, ctx):
    return pltpu.make_async_remote_copy(
        src_ref=src,
        dst_ref=dst,
        send_sem=ssem,
        recv_sem=rsem,
        device_id=(dp, ctx),
        device_id_type=pl.DeviceIdType.MESH,
    )


def signal(sem, dp, ctx):
    pl.semaphore_signal(
        sem, inc=1, device_id=(dp, ctx), device_id_type=pl.DeviceIdType.MESH
    )


def window(dp, share):
    return pl.multiple_of((dp * share) // 128 * 128, 128)


def head_lanes(head):
    lane = lax.broadcasted_iota(I32, (1, head), 1)
    return jnp.where(lane < head // 2, -1.0, 1.0).astype(F32)


def normrope(u, gain, c, s):
    inv = lax.rsqrt(jnp.mean(u * u, axis=-1, keepdims=True) + epsilon)
    v = u * inv * gain
    return v * c + pltpu.roll(v, u.shape[-1] // 2, 1) * s


def normrope_back(u, gz, gain, c, s):
    inv = lax.rsqrt(jnp.mean(u * u, axis=-1, keepdims=True) + epsilon)
    hat = u * inv
    gn = (gz * c - pltpu.roll(gz, u.shape[-1] // 2, 1) * s) * gain
    return inv * (gn - hat * jnp.mean(gn * hat, axis=-1, keepdims=True))


def far(d, n_z):
    return n_z == 8 and d in (3, 5)


def arrive_kernel(
    sizes, q, g, k, h, w, index, gain_q, gain_k, table,
    q_o, g_o, k_o, index_o, hf_o, cs, sn, kn, qs, vs,
    h_v, w_v, v_v, v_o, c0t, s0t, qg_ref, kg_ref, tab, ssem, rsem, ysem, yrem, isem, irem, hssem, hrsem, lsem,
):
    n_dp, n_x, n_y, rows, width, head, share, win = sizes
    n_ctx, n_z = n_x * n_y, n_dp // 2
    dp, me = lax.axis_index("dp"), lax.axis_index("ctx")
    x, y, z, core = me // n_y, me % n_y, dp // 2, dp % 2

    load_h = pltpu.make_async_copy(h, h_v, lsem.at[0])
    load_w = pltpu.make_async_copy(w, w_v, lsem.at[1])
    load_h.start()
    load_w.start()
    small = [
        pltpu.make_async_copy(a, b, lsem.at[8 + n])
        for n, (a, b) in enumerate(((gain_q, qg_ref), (gain_k, kg_ref), (table, tab)))
    ]
    for copy in small:
        copy.start()

    barrier = pltpu.get_barrier_semaphore()

    @pl.loop(1, n_ctx)
    def _(d):
        signal(barrier, dp, lax.rem(me + d, n_ctx))

    @pl.loop(1, n_dp)
    def _(d):
        signal(barrier, lax.rem(dp + d, n_dp), me)

    pl.semaphore_wait(barrier, n_ctx - 1 + n_dp - 1)

    def cols(s, size):
        return pl.ds(pl.multiple_of(s * size, size), size)

    def on_x(kind, d, to, frm):
        src, dst = (
            (k.at[:, cols(to, head)], k_o.at[y, frm]),
            (q.at[:, cols(to, width)], q_o.at[frm]),
            (v_v.at[:, cols(to, head)], v_o.at[y, frm]),
            (g.at[:, cols(to, width)], g_o.at[frm]),
        )[kind]
        if d == 0:
            return pltpu.make_async_copy(src, dst, lsem.at[2 + kind])
        return send(src, dst, ssem.at[kind, d], rsem.at[kind, d], dp, to * n_y + y)

    def on_y(kind, d, to, frm):
        ref = (k_o, v_o)[kind]
        return send(ref.at[frm], ref.at[frm], ysem.at[kind, d], yrem.at[kind, d], dp, x * n_y + to)

    def start_x(kind):
        for d in (*range(1, n_x), 0):
            on_x(kind, d, lax.rem(x + d, n_x), x).start()

    def arrived_x(kind):
        on_x(kind, 0, x, x).wait()
        for d in range(1, n_x):
            on_x(kind, d, x, lax.rem(x + n_x - d, n_x)).wait_recv()

    def start_y(kind):
        for d in range(1, n_y):
            on_y(kind, d, lax.rem(y + d, n_y), y).start()

    def idx_copy(d, to, frm):
        return send(index, index_o.at[frm], isem.at[d], irem.at[d], dp, to)

    def hf_copy(i, to, frm):
        return send(
            h.at[:, pl.ds(window(to, share), win)], hf_o.at[frm], hssem.at[i], hrsem.at[i], to, me
        )

    def hf_pairs():
        for d in range(n_z):
            for c in range(2):
                if (d or c) and not far(d, n_z):
                    flip = (core + c) % 2
                    yield (
                        d * 2 + c,
                        lax.rem(z + d, n_z) * 2 + flip,
                        lax.rem(z + n_z - d, n_z) * 2 + flip,
                    )

    start_x(0)
    start_x(1)

    @pl.loop(1, n_ctx)
    def _(d):
        idx_copy(d, lax.rem(me + d, n_ctx), me).start()

    own_idx = pltpu.make_async_copy(index, index_o.at[me], lsem.at[6])
    own_idx.start()
    for i, to, frm in hf_pairs():
        hf_copy(i, to, dp).start()
    load_h.wait()
    own_hf = pltpu.make_async_copy(
        h_v.at[:, pl.ds(window(dp, share), win)], hf_o.at[dp], lsem.at[7]
    )
    own_hf.start()
    load_w.wait()
    v_v[...] = dot(h_v[...], w_v[...]).astype(BF16)
    start_x(2)
    start_x(3)
    arrived_x(0)
    start_y(0)

    @pl.loop(1, n_ctx)
    def _(d):
        idx_copy(d, me, lax.rem(me + n_ctx - d, n_ctx)).wait_recv()

    own_idx.wait()
    for copy in small:
        copy.wait()

    n_docs = c0t.shape[0] // n_ctx
    ids = index_o[:, 1, :]
    bounds = [
        jnp.sum(jnp.sum((ids < d).astype(F32), axis=1, keepdims=True), axis=0, keepdims=True).astype(I32)
        for d in range(1, n_docs)
    ]
    line = lax.broadcasted_iota(I32, (n_ctx * n_docs, 1), 0)
    doc = line % n_docs
    first = jnp.zeros_like(line)
    for d, b in enumerate(bounds):
        first = jnp.where(doc == d + 1, b, first)
    angle = ((line // n_docs) * rows - first).astype(F32) * tab[2 * rows : 2 * rows + 1, :]
    c0t[...] = jnp.cos(angle)
    s0t[...] = jnp.sin(angle)
    sign = head_lanes(head)

    def block(i):
        return pl.ds(pl.multiple_of(i * rows, rows), rows)

    @pl.loop(0, n_ctx)
    def _(i):
        at = block(i)
        row = lax.broadcasted_iota(I32, (rows, 1), 0) + i * rows
        c0 = jnp.broadcast_to(c0t[pl.ds(i * n_docs, 1), :], (rows, head))
        s0 = jnp.broadcast_to(s0t[pl.ds(i * n_docs, 1), :], (rows, head))
        for d, b in enumerate(bounds):
            c0 = jnp.where(row >= b, c0t[pl.ds(i * n_docs + d + 1, 1), :], c0)
            s0 = jnp.where(row >= b, s0t[pl.ds(i * n_docs + d + 1, 1), :], s0)
        clo, slo = tab[:rows, :], tab[rows : 2 * rows, :]
        cs[at, :] = clo * c0 - slo * s0
        sn[at, :] = (slo * c0 + clo * s0) * sign

    arrived_x(1)

    @pl.loop(0, n_x)
    def _(m):
        at = block(m * n_y + y)
        c, s = cs[at, :], sn[at, :]
        for hd in range(width // head):
            u = q_o[m, :, hd * head : (hd + 1) * head].astype(F32)
            qs[m, hd * rows : (hd + 1) * rows, :] = normrope(u, qg_ref[...], c, s).astype(BF16)

    arrived_x(2)
    start_y(1)
    for d in range(1, n_y):
        on_y(0, d, y, lax.rem(y + n_y - d, n_y)).wait_recv()

    @pl.loop(0, n_ctx)
    def _(i):
        at = block(i)
        u = k_o[i % n_y, i // n_y].astype(F32)
        kn[at, :] = normrope(u, kg_ref[...], cs[at, :], sn[at, :]).astype(BF16)

    for d in range(1, n_y):
        on_y(1, d, y, lax.rem(y + n_y - d, n_y)).wait_recv()
    dest = jnp.concatenate(
        [index_o[m * n_y + f, :1, :] for f in range(n_y) for m in range(n_x)], axis=1
    )
    slab = n_ctx * rows

    @pl.loop(0, slab // TILE)
    def _(i):
        at = pl.ds(pl.multiple_of(i * TILE, TILE), TILE)
        row = lax.broadcasted_iota(I32, (TILE, 1), 0) + i * TILE
        placing = jnp.where(row == dest, 1.0, 0.0).astype(BF16)
        vs[at, :] = dot(placing, v_o[...].reshape(slab, head)).astype(BF16)

    own_hf.wait()
    arrived_x(3)
    for kind in range(2):
        for d in range(1, n_y):
            on_y(kind, d, lax.rem(y + d, n_y), y).wait_send()
    for kind in range(4):
        for d in range(1, n_x):
            on_x(kind, d, lax.rem(x + d, n_x), x).wait_send()

    @pl.loop(1, n_ctx)
    def _(d):
        idx_copy(d, lax.rem(me + d, n_ctx), me).wait_send()

    for i, to, frm in hf_pairs():
        hf_copy(i, to, dp).wait_send()
        hf_copy(i, dp, frm).wait_recv()


def attend_kernel(
    sizes, qs, g_ref, kn, vs, index_ref,
    gq_ref, gk_ref, gv_ref, ga_ref,
    gs, es, ds_, gv_acc, gvt,
):
    n_x, n_y, rows, heads, head, n_docs = sizes
    slab = n_x * n_y * rows
    blocks = slab // rows
    factor = head ** (-0.5)
    y = lax.axis_index("ctx") % n_y

    ids = index_ref[:, 1, :]
    bounds = [jnp.sum((ids < d).astype(F32)).astype(I32) for d in range(1, n_docs)]

    def start_of(row):
        start = jnp.zeros_like(row)
        for b in bounds:
            start = jnp.where(row >= b, b, start)
        return start

    def block(i):
        return pl.ds(pl.multiple_of(i * rows, rows), rows)

    gk_ref[...] = jnp.zeros_like(gk_ref)
    gv_acc[...] = jnp.zeros_like(gv_acc)
    for m in range(n_x):
        for hd in range(heads):
            gs[m, hd * rows : (hd + 1) * rows, :] = g_ref[m, :, hd * head : (hd + 1) * head]

    scale = factor * math.log2(math.e)
    part = heads * rows // 2

    @pl.loop(0, n_x)
    def _(m):
        i = m * n_y + y
        r0 = pl.multiple_of(i * rows, rows)
        row = lax.broadcasted_iota(I32, (1, rows), 1) + r0
        start = start_of(row)
        first = jnp.zeros((), I32)
        for b in bounds:
            first = jnp.where(r0 >= b, b, first)
        low, high = first // TILE, (r0 + rows - 1) // TILE + 1

        def forward(j, carry):
            k0 = pl.multiple_of(j * TILE, TILE)
            at = pl.ds(k0, TILE)
            key = lax.broadcasted_iota(I32, (TILE, 1), 0) + k0
            allowed = (key >= start) & (key <= row)
            sums = []
            for n in range(2):
                here = slice(n * part, (n + 1) * part)
                logits = dot(kn[at, :], qs[m, here, :], NT) * scale
                pg = dot(vs[at, :], gs[m, here, :], NT)
                e = jnp.concatenate(
                    [
                        jnp.where(allowed, jnp.exp2(logits[:, c : c + rows]), 0.0)
                        for c in range(0, part, rows)
                    ],
                    axis=1,
                )
                es[j, :, here] = e
                ds_[j, :, here] = pg
                sums.append(carry[2 * n] + jnp.sum(e, axis=0, keepdims=True))
                sums.append(carry[2 * n + 1] + jnp.sum(e * pg, axis=0, keepdims=True))
            return tuple(sums)

        zero = jnp.zeros((1, part), F32)
        sums = lax.fori_loop(low, high, forward, (zero,) * 4)
        inv = [1.0 / sums[0], 1.0 / sums[2]]
        delta = [sums[1] * inv[0], sums[3] * inv[1]]
        gq_ref[m] = jnp.zeros((heads * rows, head), F32)

        @pl.loop(low, high)
        def _(j):
            at = pl.ds(pl.multiple_of(j * TILE, TILE), TILE)
            for n in range(2):
                here = slice(n * part, (n + 1) * part)
                p = es[j, :, here] * inv[n]
                dsj = (p * (ds_[j, :, here] - delta[n])).astype(BF16)
                gk_ref[at, :] += dot(dsj, qs[m, here, :])
                gv_acc[at, :] += dot(p.astype(BF16), gs[m, here, :])
                gq_ref[m, here, :] += dot(dsj, kn[at, :], TN)

    @pl.loop(0, blocks)
    def _(i):
        gv = gv_acc[block(i), :]
        gv_ref[i % n_y, i // n_y] = gv.astype(BF16)
        gvt[:, block(i)] = gv.T.astype(BF16)

    for f in range(n_y):
        for m in range(0, n_x, 2):
            dest = jnp.concatenate(
                [index_ref[(m + n) * n_y + f, :1, :] for n in range(2)], axis=1
            )
            row = lax.broadcasted_iota(I32, (slab, 1), 0)
            picking = jnp.where(row == dest, 1.0, 0.0).astype(BF16)
            moved = dot(gvt[...], picking).T.astype(BF16)
            for n in range(2):
                ga_ref[f, m + n] = moved[n * rows : (n + 1) * rows]


def return_kernel(
    sizes, gq_raw, gk_raw, gv, ga, w, h, hf, q_in, k_in, cs, sn, qg_ref, kg_ref,
    gq_o, gk_o, h_o, w_o,
    gq, gk, r1, s1, r2, vg, ag, w_v, hf_v, hft, dw, dws, dwr,
    qsem, qrem, ysem, yrem, xsem, xrem, lsem, ag_s, ag_r, ws, wr, hssem, hrsem,
):
    n_dp, n_x, n_y, rows, width, head, share, win = sizes
    n_ctx, n_z = n_x * n_y, n_dp // 2
    dp, me = lax.axis_index("dp"), lax.axis_index("ctx")
    x, y, z, core = me // n_y, me % n_y, dp // 2, dp % 2
    after = lax.rem(z + 1, n_z) * 2 + core
    before = lax.rem(z + n_z - 1, n_z) * 2 + core
    twin = z * 2 + 1 - core
    ahead = n_z // 2
    behind = n_z - 1 - ahead

    load_w = pltpu.make_async_copy(w, w_v, lsem.at[0])
    load_w.start()
    dws[...] = jnp.zeros_like(dws)

    def hf_pairs(away):
        for d in range(n_z):
            for c in range(2):
                if far(d, n_z) == away:
                    flip = (core + c) % 2
                    yield (
                        d * 2 + c,
                        lax.rem(z + d, n_z) * 2 + flip,
                        lax.rem(z + n_z - d, n_z) * 2 + flip,
                    )

    hf_loads = [
        pltpu.make_async_copy(hf.at[frm], hf_v.at[frm], hrsem.at[i])
        for i, _, frm in hf_pairs(False)
    ]
    for copy in hf_loads:
        copy.start()

    barrier = pltpu.get_barrier_semaphore()

    @pl.loop(1, n_ctx)
    def _(d):
        signal(barrier, dp, lax.rem(me + d, n_ctx))

    @pl.loop(1, n_dp)
    def _(d):
        signal(barrier, lax.rem(dp + d, n_dp), me)

    pl.semaphore_wait(barrier, n_ctx - 1 + n_dp - 1)

    grads = (ga, gv, gk)

    def on_y(kind, d, to, frm):
        src, dst = grads[kind].at[to], r1.at[kind, frm]
        if d == 0:
            return pltpu.make_async_copy(src, dst, lsem.at[1 + kind])
        return send(src, dst, ysem.at[kind, d], yrem.at[kind, d], dp, x * n_y + to)

    def on_x(kind, d, to, frm):
        dst = ag.at[dp, frm] if kind == 0 else r2.at[kind - 1, frm]
        return send(s1.at[kind, to], dst, xsem.at[kind, d], xrem.at[kind, d], dp, to * n_y + y)

    def q_copy(n, d, to, frm):
        part = width // 2
        src = gq.at[to, :, pl.ds(n * part, part)]
        dst = gq_o.at[:, pl.ds(pl.multiple_of(frm * width + n * part, part), part)]
        if d == 0:
            return pltpu.make_async_copy(src, dst, lsem.at[4 + n])
        return send(src, dst, qsem.at[n, d], qrem.at[n, d], dp, to * n_y + y)

    def hf_copy(i, to, frm):
        return send(
            h.at[:, pl.ds(window(to, share), win)], hf_v.at[frm], hssem.at[i], hrsem.at[i], to, me
        )

    def start_y(kind):
        for d in (*range(1, n_y), 0):
            on_y(kind, d, lax.rem(y + d, n_y), y).start()

    def start_q(n):
        for d in (*range(1, n_x), 0):
            q_copy(n, d, lax.rem(x + d, n_x), x).start()

    def reduce_y(kind):
        on_y(kind, 0, y, y).wait()
        for d in range(1, n_y):
            on_y(kind, d, y, lax.rem(y + n_y - d, n_y)).wait_recv()
        for m in range(n_x):
            total = r1[kind, 0, m].astype(F32)
            for f in range(1, n_y):
                total = total + r1[kind, f, m].astype(F32)
            s1[kind, m] = total.astype(BF16)

    def start_x(kind):
        for d in range(1, n_x):
            on_x(kind, d, lax.rem(x + d, n_x), x).start()

    def arrived_x(kind):
        for d in range(1, n_x):
            on_x(kind, d, x, lax.rem(x + n_x - d, n_x)).wait_recv()

    start_y(0)
    for i, to, frm in hf_pairs(True):
        hf_copy(i, to, dp).start()
    factor = head ** (-0.5)

    @pl.loop(0, n_x)
    def _(m):
        at = pl.ds(pl.multiple_of((m * n_y + y) * rows, rows), rows)
        c, s = cs[at, :], sn[at, :]
        for hd in range(width // head):
            lanes = slice(hd * head, (hd + 1) * head)
            gz = gq_raw[m, hd * rows : (hd + 1) * rows, :] * factor
            u = q_in[m, :, lanes].astype(F32)
            gq[m, :, lanes] = normrope_back(u, gz, qg_ref[...], c, s).astype(BF16)

    start_q(0)
    start_y(1)

    @pl.loop(0, n_ctx)
    def _(i):
        at = pl.ds(pl.multiple_of(i * rows, rows), rows)
        gz = gk_raw[at, :] * factor
        u = k_in[i % n_y, i // n_y].astype(F32)
        gk[i % n_y, i // n_y] = normrope_back(u, gz, kg_ref[...], cs[at, :], sn[at, :]).astype(BF16)

    reduce_y(0)
    start_x(0)
    start_y(2)
    start_q(1)
    ag[dp, x] = s1[0, x]
    for copy in hf_loads:
        copy.wait()
    for i, _, frm in hf_pairs(False):
        hft[frm] = hf_v[frm].T
    arrived_x(0)

    def piece(slot, ch):
        return ag.at[slot, ch]

    def takes(t, ch, way):
        return t <= behind or (t == ahead and (ch < n_x // 2) == (way == 0))

    def ring(slot, ch, way, to):
        return send(piece(slot, ch), piece(slot, ch), ag_s.at[slot, way, ch], ag_r.at[slot, ch], to, me)

    sent = []

    def go(slot, ch, way, to):
        copy = ring(slot, ch, way, to)
        copy.start()
        sent.append(copy)

    for ch in range(n_x):
        if takes(1, ch, 0):
            go(dp, ch, 0, after)
        if takes(1, ch, 1):
            go(dp, ch, 1, before)
    for ch in range(n_x):
        go(dp, ch, 2, twin)

    def relay(t):
        for ch in range(n_x):
            for way, to, hop in ((0, after, n_z - t), (1, before, t)):
                if takes(t, ch, way):
                    slot = lax.rem(z + hop, n_z) * 2 + core
                    ring(slot, ch, way, to).wait_recv()
                    if takes(t + 1, ch, way):
                        go(slot, ch, way, to)
                    go(slot, ch, 2, twin)

    started = [False]

    def weigh(d):
        slots = [lax.rem(z + d, n_z) * 2 + c for c in (core, 1 - core)]
        for ch in range(n_x):
            ring(slots[1], ch, 2, twin).wait_recv()
        a = jnp.concatenate([hft[e] for e in slots], axis=1)
        b = jnp.concatenate(
            [jnp.concatenate([ag[e, hd] for hd in range(n_x)], axis=1) for e in slots], axis=0
        )
        if started[0]:
            dw[...] += dot(a, b)
        else:
            dw[...] = dot(a, b)
            started[0] = True

    model = h_o.shape[1]
    sub = 256

    def hidden_part(n, parts):
        span = model // parts

        @pl.loop(0, span // sub)
        def _(i):
            at = pl.ds(pl.multiple_of(n * span + i * sub, sub), sub)
            h_o[:, at] = dot(vg[...], w_v[at, :], NT).astype(BF16)

    def first_half():
        arrived_x(1)
        for hd in range(n_x):
            vg[:, hd * head : (hd + 1) * head] = r2[0, hd]
        load_w.wait()
        hidden_part(0, 2)

    reduce_y(1)
    start_x(1)
    relay(1)
    reduce_y(2)
    start_x(2)
    r2[0, x] = s1[1, x]
    r2[1, x] = s1[2, x]
    for i, _, frm in hf_pairs(True):
        hf_copy(i, dp, frm).wait_recv()
        hft[frm] = hf_v[frm].T
    for t in range(2, ahead):
        relay(t)
        if t == 2:
            weigh(0)
            first_half()
        else:
            for d in (1, 2) if t == 3 else (t - 1,):
                weigh(d)
                weigh(n_z - d)
    if ahead > 1:
        relay(ahead)
    for d in range(ahead - 1, n_z - ahead + 2) if ahead > 2 else range(n_z):
        weigh(d)
    if ahead < 3:
        first_half()

    off = pl.multiple_of(dp * share - (dp * share) // 128 * 128, 64)
    out_rows = share // n_ctx
    for o in range(0, win - share + 1, 64):

        @pl.when(off == o)
        def _(o=o):
            for c in range(n_ctx):
                at = slice(o + c * out_rows, o + (c + 1) * out_rows)
                dws[c, :out_rows, :] = dw[at, :].astype(BF16)

    def w_copy(d, to, frm):
        return send(dws.at[to], dwr.at[frm], ws.at[d], wr.at[d], dp, to)

    @pl.loop(1, n_ctx)
    def _(d):
        w_copy(d, lax.rem(me + d, n_ctx), me).start()

    dwr[me] = dws[me]
    hidden_part(1, 2)
    arrived_x(2)
    for hd in range(n_x):
        gk_o[:, hd * head : (hd + 1) * head] = r2[1, hd]
    for n in range(2):
        q_copy(n, 0, x, x).wait()
        for d in range(1, n_x):
            q_copy(n, d, x, lax.rem(x + n_x - d, n_x)).wait_recv()
            q_copy(n, d, lax.rem(x + d, n_x), x).wait_send()
    for copy in sent:
        copy.wait_send()
    for kind in range(3):
        for d in range(1, n_y):
            on_y(kind, d, lax.rem(y + d, n_y), y).wait_send()
        for d in range(1, n_x):
            on_x(kind, d, lax.rem(x + d, n_x), x).wait_send()
    for i, to, _ in hf_pairs(True):
        hf_copy(i, to, dp).wait_send()

    @pl.loop(1, n_ctx)
    def _(d):
        w_copy(d, me, lax.rem(me + n_ctx - d, n_ctx)).wait_recv()

    total = dwr[0].astype(F32)
    for c in range(1, n_ctx):
        total = total + dwr[c].astype(F32)
    w_o[...] = total[:out_rows] * (1.0 / (n_dp * n_ctx))

    @pl.loop(1, n_ctx)
    def _(d):
        w_copy(d, lax.rem(me + d, n_ctx), me).wait_send()


def on_device(hidden, queries, key_states, out_grad, w_value, q_gain, k_gain, dest_rows, doc_ids):
    n_dp, n_ctx = lax.axis_size("dp"), lax.axis_size("ctx")
    rows, model = hidden.shape[1:]
    head = q_gain.shape[0]
    kv_width = key_states.shape[2]
    n_x = kv_width // head
    n_y = n_ctx // n_x
    width = queries.shape[2] // n_x
    heads = width // head
    slab = rows * n_ctx
    share = model // n_dp
    win = (share + 127) // 128 * 128
    sizes = (n_dp, n_x, n_y, rows, width, head, share, win)
    sds = jax.ShapeDtypeStruct
    dma = pltpu.SemaphoreType.DMA

    index = jnp.concatenate([dest_rows, doc_ids], axis=0)
    wide = sds((n_x, rows, width), BF16)
    narrow = sds((n_y, n_x, rows, head), BF16)
    half = head // 2
    frequency = rope_base ** (-(np.arange(half, dtype=np.float64) * 2.0 / head))
    frequency = np.concatenate([frequency, frequency])[None]
    low = np.arange(rows, dtype=np.float64)[:, None] * frequency
    table = np.concatenate([np.cos(low), np.sin(low), np.repeat(frequency, 8, axis=0)])
    table = jnp.asarray(table, F32)
    n_docs = 4
    stacked = (n_x, heads * rows, head)
    flat = sds((slab, head), BF16)
    kept = [
        pltpu.with_memory_space_constraint(a, pltpu.HBM)
        for a in (queries[0], out_grad[0], key_states[0], hidden[0], w_value)
    ]
    tail = [
        pltpu.with_memory_space_constraint(a, pltpu.HBM)
        for a in (q_gain[None], k_gain[None], table)
    ]
    q_in, g_in, k_in, index_in, hf, cs, sn, kn, qs, vs = pl.pallas_call(
        functools.partial(arrive_kernel, sizes),
        out_shape=(
            wide,
            wide,
            narrow,
            sds((n_ctx, 2, rows), I32),
            sds((n_dp, rows, win), BF16),
            sds((slab, head), F32),
            sds((slab, head), F32),
            flat,
            sds(stacked, BF16),
            flat,
        ),
        in_specs=[HBM] * 5 + [ANY] + [HBM] * 3,
        out_specs=(VMEM, ANY, VMEM, VMEM, ANY) + (VMEM,) * 5,
        scratch_shapes=[
            pltpu.VMEM((rows, model), BF16),
            pltpu.VMEM((model, kv_width), BF16),
            pltpu.VMEM((rows, kv_width), BF16),
            pltpu.VMEM((n_y, n_x, rows, head), BF16),
            pltpu.VMEM((n_ctx * n_docs, head), F32),
            pltpu.VMEM((n_ctx * n_docs, head), F32),
            pltpu.VMEM((1, head), F32),
            pltpu.VMEM((1, head), F32),
            pltpu.VMEM((2 * rows + 8, head), F32),
            dma((4, n_x)),
            dma((4, n_x)),
            dma((2, n_y)),
            dma((2, n_y)),
            dma((n_ctx,)),
            dma((n_ctx,)),
            dma((n_dp,)),
            dma((n_dp,)),
            dma((11,)),
        ],
        compiler_params=pltpu.CompilerParams(
            collective_id=0, has_side_effects=True, vmem_limit_bytes=24 << 20
        ),
        name="arrive",
    )(*kept, index, *tail)

    tiles = slab // TILE
    gq, gk, gv, ga = pl.pallas_call(
        functools.partial(attend_kernel, (n_x, n_y, rows, heads, head, n_docs)),
        out_shape=(sds(stacked, F32), sds((slab, head), F32), narrow, narrow),
        in_specs=[VMEM] * 5,
        out_specs=(VMEM,) * 4,
        scratch_shapes=[
            pltpu.VMEM(stacked, BF16),
            pltpu.VMEM((tiles, TILE, heads * rows), F32),
            pltpu.VMEM((tiles, TILE, heads * rows), F32),
            pltpu.VMEM((slab, head), F32),
            pltpu.VMEM((head, slab), BF16),
        ],
        compiler_params=pltpu.CompilerParams(vmem_limit_bytes=36 << 20),
        name="attend",
    )(qs, g_in, kn, vs, index_in)

    out_rows = share // n_ctx
    pad = (out_rows + 15) // 16 * 16
    results = (
        sds((rows, n_x * width), BF16),
        sds((rows, kv_width), BF16),
        sds((rows, model), BF16),
        sds((out_rows, kv_width), F32),
    )
    query_grad, key_grad, hidden_grad, weight_grad = pl.pallas_call(
        functools.partial(return_kernel, sizes),
        out_shape=results,
        in_specs=[VMEM] * 2 + [ANY] * 2 + [HBM] * 2 + [ANY] + [VMEM] * 6,
        out_specs=(ANY, VMEM, VMEM, VMEM),
        scratch_shapes=[
            pltpu.VMEM((n_x, rows, width), BF16),
            pltpu.VMEM((n_y, n_x, rows, head), BF16),
            pltpu.VMEM((3, n_y, n_x, rows, head), BF16),
            pltpu.VMEM((3, n_x, rows, head), BF16),
            pltpu.VMEM((2, n_x, rows, head), BF16),
            pltpu.VMEM((rows, kv_width), BF16),
            pltpu.VMEM((n_dp, n_x, rows, head), BF16),
            pltpu.VMEM((model, kv_width), BF16),
            pltpu.VMEM((n_dp, rows, win), BF16),
            pltpu.VMEM((n_dp, win, rows), BF16),
            pltpu.VMEM((win, kv_width), F32),
            pltpu.VMEM((n_ctx, pad, kv_width), BF16),
            pltpu.VMEM((n_ctx, pad, kv_width), BF16),
            dma((2, n_x)),
            dma((2, n_x)),
            dma((3, n_y)),
            dma((3, n_y)),
            dma((3, n_x)),
            dma((3, n_x)),
            dma((6,)),
            dma((n_dp, 3, n_x)),
            dma((n_dp, n_x)),
            dma((n_ctx,)),
            dma((n_ctx,)),
            dma((n_dp,)),
            dma((n_dp,)),
        ],
        compiler_params=pltpu.CompilerParams(
            collective_id=1, has_side_effects=True, vmem_limit_bytes=32 << 20
        ),
        name="give_back",
    )(gq, gk, gv, ga, w_value, hidden[0], hf, q_in, k_in, cs, sn, q_gain[None], k_gain[None])
    return (hidden_grad[None], query_grad[None], key_grad[None], weight_grad)


def solution(mesh):
    rows = P("dp", "ctx", None)
    return jax.shard_map(
        on_device,
        mesh=mesh,
        in_specs=(rows, rows, rows, rows, P(), P(), P(), P("dp", "ctx"), P("dp", "ctx")),
        out_specs=(rows, rows, rows, P(("dp", "ctx"), None)),
        check_vma=False,
    )
```

```python
import functools
import math

import jax
import jax.numpy as jnp
import numpy as np
from jax import lax
from jax.experimental import pallas as pl
from jax.experimental.pallas import tpu as pltpu
from jax.sharding import PartitionSpec as P

epsilon = 1e-06
rope_base = 1000000.0
BF16, F32, I32 = jnp.bfloat16, jnp.float32, jnp.int32
ANY = pl.BlockSpec(memory_space=pl.ANY)
HBM = pl.BlockSpec(memory_space=pltpu.HBM)
VMEM = pl.BlockSpec(memory_space=pltpu.VMEM)
TILE = 256
NT = (((1,), (1,)), ((), ()))
TN = (((0,), (0,)), ((), ()))


def dot(a, b, dims=(((1,), (0,)), ((), ()))):
    return lax.dot_general(a, b, dims, preferred_element_type=F32)


def send(src, dst, ssem, rsem, dp, ctx):
    return pltpu.make_async_remote_copy(
        src_ref=src,
        dst_ref=dst,
        send_sem=ssem,
        recv_sem=rsem,
        device_id=(dp, ctx),
        device_id_type=pl.DeviceIdType.MESH,
    )


def signal(sem, dp, ctx):
    pl.semaphore_signal(
        sem, inc=1, device_id=(dp, ctx), device_id_type=pl.DeviceIdType.MESH
    )


def window(dp, share):
    return pl.multiple_of((dp * share) // 128 * 128, 128)


def head_lanes(head):
    lane = lax.broadcasted_iota(I32, (1, head), 1)
    return jnp.where(lane < head // 2, -1.0, 1.0).astype(F32)


def normrope(u, gain, c, s):
    inv = lax.rsqrt(jnp.mean(u * u, axis=-1, keepdims=True) + epsilon)
    v = u * inv * gain
    return v * c + pltpu.roll(v, u.shape[-1] // 2, 1) * s


def normrope_back(u, gz, gain, c, s):
    inv = lax.rsqrt(jnp.mean(u * u, axis=-1, keepdims=True) + epsilon)
    hat = u * inv
    gn = (gz * c - pltpu.roll(gz, u.shape[-1] // 2, 1) * s) * gain
    return inv * (gn - hat * jnp.mean(gn * hat, axis=-1, keepdims=True))


def far(d, n_z):
    return n_z == 8 and d in (3, 5)


def arrive_kernel(
    sizes, q, g, k, h, w, index, gain_q, gain_k, table,
    q_o, g_o, k_o, index_o, hf_o, cs, sn, kn, qs, vs,
    h_v, w_v, v_v, v_o, c0t, s0t, qg_ref, kg_ref, tab, ssem, rsem, ysem, yrem, isem, irem, hssem, hrsem, lsem,
):
    n_dp, n_x, n_y, rows, width, head, share, win = sizes
    n_ctx, n_z = n_x * n_y, n_dp // 2
    dp, me = lax.axis_index("dp"), lax.axis_index("ctx")
    x, y, z, core = me // n_y, me % n_y, dp // 2, dp % 2

    load_h = pltpu.make_async_copy(h, h_v, lsem.at[0])
    load_w = pltpu.make_async_copy(w, w_v, lsem.at[1])
    load_h.start()
    load_w.start()
    small = [
        pltpu.make_async_copy(a, b, lsem.at[8 + n])
        for n, (a, b) in enumerate(((gain_q, qg_ref), (gain_k, kg_ref), (table, tab)))
    ]
    for copy in small:
        copy.start()

    barrier = pltpu.get_barrier_semaphore()

    @pl.loop(1, n_ctx)
    def _(d):
        signal(barrier, dp, lax.rem(me + d, n_ctx))

    @pl.loop(1, n_dp)
    def _(d):
        signal(barrier, lax.rem(dp + d, n_dp), me)

    pl.semaphore_wait(barrier, n_ctx - 1 + n_dp - 1)

    def cols(s, size):
        return pl.ds(pl.multiple_of(s * size, size), size)

    def on_x(kind, d, to, frm):
        src, dst = (
            (k.at[:, cols(to, head)], k_o.at[y, frm]),
            (q.at[:, cols(to, width)], q_o.at[frm]),
            (v_v.at[:, cols(to, head)], v_o.at[y, frm]),
            (g.at[:, cols(to, width)], g_o.at[frm]),
        )[kind]
        if d == 0:
            return pltpu.make_async_copy(src, dst, lsem.at[2 + kind])
        return send(src, dst, ssem.at[kind, d], rsem.at[kind, d], dp, to * n_y + y)

    def on_y(kind, d, to, frm):
        ref = (k_o, v_o)[kind]
        return send(ref.at[frm], ref.at[frm], ysem.at[kind, d], yrem.at[kind, d], dp, x * n_y + to)

    def start_x(kind):
        for d in (*range(1, n_x), 0):
            on_x(kind, d, lax.rem(x + d, n_x), x).start()

    def arrived_x(kind):
        on_x(kind, 0, x, x).wait()
        for d in range(1, n_x):
            on_x(kind, d, x, lax.rem(x + n_x - d, n_x)).wait_recv()

    def start_y(kind):
        for d in range(1, n_y):
            on_y(kind, d, lax.rem(y + d, n_y), y).start()

    def idx_copy(d, to, frm):
        return send(index, index_o.at[frm], isem.at[d], irem.at[d], dp, to)

    def hf_copy(i, to, frm):
        return send(
            h.at[:, pl.ds(window(to, share), win)], hf_o.at[frm], hssem.at[i], hrsem.at[i], to, me
        )

    def hf_pairs():
        for d in range(n_z):
            for c in range(2):
                if (d or c) and not far(d, n_z):
                    flip = (core + c) % 2
                    yield (
                        d * 2 + c,
                        lax.rem(z + d, n_z) * 2 + flip,
                        lax.rem(z + n_z - d, n_z) * 2 + flip,
                    )

    start_x(0)
    start_x(1)

    @pl.loop(1, n_ctx)
    def _(d):
        idx_copy(d, lax.rem(me + d, n_ctx), me).start()

    own_idx = pltpu.make_async_copy(index, index_o.at[me], lsem.at[6])
    own_idx.start()
    for i, to, frm in hf_pairs():
        hf_copy(i, to, dp).start()
    load_h.wait()
    own_hf = pltpu.make_async_copy(
        h_v.at[:, pl.ds(window(dp, share), win)], hf_o.at[dp], lsem.at[7]
    )
    own_hf.start()
    load_w.wait()
    v_v[...] = dot(h_v[...], w_v[...]).astype(BF16)
    start_x(2)
    start_x(3)
    arrived_x(0)
    start_y(0)

    @pl.loop(1, n_ctx)
    def _(d):
        idx_copy(d, me, lax.rem(me + n_ctx - d, n_ctx)).wait_recv()

    own_idx.wait()
    for copy in small:
        copy.wait()

    n_docs = c0t.shape[0] // n_ctx
    ids = index_o[:, 1, :]
    bounds = [
        jnp.sum(jnp.sum((ids < d).astype(F32), axis=1, keepdims=True), axis=0, keepdims=True).astype(I32)
        for d in range(1, n_docs)
    ]
    line = lax.broadcasted_iota(I32, (n_ctx * n_docs, 1), 0)
    doc = line % n_docs
    first = jnp.zeros_like(line)
    for d, b in enumerate(bounds):
        first = jnp.where(doc == d + 1, b, first)
    angle = ((line // n_docs) * rows - first).astype(F32) * tab[2 * rows : 2 * rows + 1, :]
    c0t[...] = jnp.cos(angle)
    s0t[...] = jnp.sin(angle)
    sign = head_lanes(head)

    def block(i):
        return pl.ds(pl.multiple_of(i * rows, rows), rows)

    @pl.loop(0, n_ctx)
    def _(i):
        at = block(i)
        row = lax.broadcasted_iota(I32, (rows, 1), 0) + i * rows
        c0 = jnp.broadcast_to(c0t[pl.ds(i * n_docs, 1), :], (rows, head))
        s0 = jnp.broadcast_to(s0t[pl.ds(i * n_docs, 1), :], (rows, head))
        for d, b in enumerate(bounds):
            c0 = jnp.where(row >= b, c0t[pl.ds(i * n_docs + d + 1, 1), :], c0)
            s0 = jnp.where(row >= b, s0t[pl.ds(i * n_docs + d + 1, 1), :], s0)
        clo, slo = tab[:rows, :], tab[rows : 2 * rows, :]
        cs[at, :] = clo * c0 - slo * s0
        sn[at, :] = (slo * c0 + clo * s0) * sign

    arrived_x(1)

    @pl.loop(0, n_x)
    def _(m):
        at = block(m * n_y + y)
        c, s = cs[at, :], sn[at, :]
        for hd in range(width // head):
            u = q_o[m, :, hd * head : (hd + 1) * head].astype(F32)
            qs[m, hd * rows : (hd + 1) * rows, :] = normrope(u, qg_ref[...], c, s).astype(BF16)

    arrived_x(2)
    start_y(1)
    for d in range(1, n_y):
        on_y(0, d, y, lax.rem(y + n_y - d, n_y)).wait_recv()

    @pl.loop(0, n_ctx)
    def _(i):
        at = block(i)
        u = k_o[i % n_y, i // n_y].astype(F32)
        kn[at, :] = normrope(u, kg_ref[...], cs[at, :], sn[at, :]).astype(BF16)

    for d in range(1, n_y):
        on_y(1, d, y, lax.rem(y + n_y - d, n_y)).wait_recv()
    dest = jnp.concatenate(
        [index_o[m * n_y + f, :1, :] for f in range(n_y) for m in range(n_x)], axis=1
    )
    slab = n_ctx * rows

    @pl.loop(0, slab // TILE)
    def _(i):
        at = pl.ds(pl.multiple_of(i * TILE, TILE), TILE)
        row = lax.broadcasted_iota(I32, (TILE, 1), 0) + i * TILE
        placing = jnp.where(row == dest, 1.0, 0.0).astype(BF16)
        vs[at, :] = dot(placing, v_o[...].reshape(slab, head)).astype(BF16)

    own_hf.wait()
    arrived_x(3)
    for kind in range(2):
        for d in range(1, n_y):
            on_y(kind, d, lax.rem(y + d, n_y), y).wait_send()
    for kind in range(4):
        for d in range(1, n_x):
            on_x(kind, d, lax.rem(x + d, n_x), x).wait_send()

    @pl.loop(1, n_ctx)
    def _(d):
        idx_copy(d, lax.rem(me + d, n_ctx), me).wait_send()

    for i, to, frm in hf_pairs():
        hf_copy(i, to, dp).wait_send()
        hf_copy(i, dp, frm).wait_recv()


def attend_kernel(
    sizes, qs, g_ref, kn, vs, index_ref,
    gq_ref, gk_ref, gv_ref, ga_ref,
    gs, es, ds_, gv_acc, gvt,
):
    n_x, n_y, rows, heads, head, n_docs = sizes
    slab = n_x * n_y * rows
    blocks = slab // rows
    factor = head ** (-0.5)
    y = lax.axis_index("ctx") % n_y

    ids = index_ref[:, 1, :]
    bounds = [jnp.sum((ids < d).astype(F32)).astype(I32) for d in range(1, n_docs)]

    def start_of(row):
        start = jnp.zeros_like(row)
        for b in bounds:
            start = jnp.where(row >= b, b, start)
        return start

    def block(i):
        return pl.ds(pl.multiple_of(i * rows, rows), rows)

    gk_ref[...] = jnp.zeros_like(gk_ref)
    gv_acc[...] = jnp.zeros_like(gv_acc)
    for m in range(n_x):
        for hd in range(heads):
            gs[m, hd * rows : (hd + 1) * rows, :] = g_ref[m, :, hd * head : (hd + 1) * head]

    scale = factor * math.log2(math.e)
    part = heads * rows // 2

    @pl.loop(0, n_x)
    def _(m):
        i = m * n_y + y
        r0 = pl.multiple_of(i * rows, rows)
        row = lax.broadcasted_iota(I32, (1, rows), 1) + r0
        start = start_of(row)
        first = jnp.zeros((), I32)
        for b in bounds:
            first = jnp.where(r0 >= b, b, first)
        low, high = first // TILE, (r0 + rows - 1) // TILE + 1

        def forward(j, carry):
            k0 = pl.multiple_of(j * TILE, TILE)
            at = pl.ds(k0, TILE)
            key = lax.broadcasted_iota(I32, (TILE, 1), 0) + k0
            allowed = (key >= start) & (key <= row)
            sums = []
            for n in range(2):
                here = slice(n * part, (n + 1) * part)
                logits = dot(kn[at, :], qs[m, here, :], NT) * scale
                pg = dot(vs[at, :], gs[m, here, :], NT)
                e = jnp.concatenate(
                    [
                        jnp.where(allowed, jnp.exp2(logits[:, c : c + rows]), 0.0)
                        for c in range(0, part, rows)
                    ],
                    axis=1,
                )
                es[j, :, here] = e
                ds_[j, :, here] = pg
                sums.append(carry[2 * n] + jnp.sum(e, axis=0, keepdims=True))
                sums.append(carry[2 * n + 1] + jnp.sum(e * pg, axis=0, keepdims=True))
            return tuple(sums)

        zero = jnp.zeros((1, part), F32)
        sums = lax.fori_loop(low, high, forward, (zero,) * 4)
        inv = [1.0 / sums[0], 1.0 / sums[2]]
        delta = [sums[1] * inv[0], sums[3] * inv[1]]
        gq_ref[m] = jnp.zeros((heads * rows, head), F32)

        @pl.loop(low, high)
        def _(j):
            at = pl.ds(pl.multiple_of(j * TILE, TILE), TILE)
            for n in range(2):
                here = slice(n * part, (n + 1) * part)
                p = es[j, :, here] * inv[n]
                dsj = (p * (ds_[j, :, here] - delta[n])).astype(BF16)
                gk_ref[at, :] += dot(dsj, qs[m, here, :])
                gv_acc[at, :] += dot(p.astype(BF16), gs[m, here, :])
                gq_ref[m, here, :] += dot(dsj, kn[at, :], TN)

    @pl.loop(0, blocks)
    def _(i):
        gv = gv_acc[block(i), :]
        gv_ref[i % n_y, i // n_y] = gv.astype(BF16)
        gvt[:, block(i)] = gv.T.astype(BF16)

    for f in range(n_y):
        for m in range(0, n_x, 2):
            dest = jnp.concatenate(
                [index_ref[(m + n) * n_y + f, :1, :] for n in range(2)], axis=1
            )
            row = lax.broadcasted_iota(I32, (slab, 1), 0)
            picking = jnp.where(row == dest, 1.0, 0.0).astype(BF16)
            moved = dot(gvt[...], picking).T.astype(BF16)
            for n in range(2):
                ga_ref[f, m + n] = moved[n * rows : (n + 1) * rows]


def return_kernel(
    sizes, gq_raw, gk_raw, gv, ga, w, h, hf, q_in, k_in, cs, sn, qg_ref, kg_ref,
    gq_o, gk_o, h_o, w_o,
    gq, gk, r1, s1, r2, vg, ag, w_v, hf_v, hft, dw, dws, dwr,
    qsem, qrem, ysem, yrem, xsem, xrem, lsem, ag_s, ag_r, ws, wr, hssem, hrsem,
):
    n_dp, n_x, n_y, rows, width, head, share, win = sizes
    n_ctx, n_z = n_x * n_y, n_dp // 2
    dp, me = lax.axis_index("dp"), lax.axis_index("ctx")
    x, y, z, core = me // n_y, me % n_y, dp // 2, dp % 2
    after = lax.rem(z + 1, n_z) * 2 + core
    before = lax.rem(z + n_z - 1, n_z) * 2 + core
    twin = z * 2 + 1 - core
    ahead = n_z // 2
    behind = n_z - 1 - ahead

    load_w = pltpu.make_async_copy(w, w_v, lsem.at[0])
    load_w.start()
    dws[...] = jnp.zeros_like(dws)

    def hf_pairs(away):
        for d in range(n_z):
            for c in range(2):
                if far(d, n_z) == away:
                    flip = (core + c) % 2
                    yield (
                        d * 2 + c,
                        lax.rem(z + d, n_z) * 2 + flip,
                        lax.rem(z + n_z - d, n_z) * 2 + flip,
                    )

    hf_loads = [
        pltpu.make_async_copy(hf.at[frm], hf_v.at[frm], hrsem.at[i])
        for i, _, frm in hf_pairs(False)
    ]
    for copy in hf_loads:
        copy.start()

    barrier = pltpu.get_barrier_semaphore()

    @pl.loop(1, n_ctx)
    def _(d):
        signal(barrier, dp, lax.rem(me + d, n_ctx))

    @pl.loop(1, n_dp)
    def _(d):
        signal(barrier, lax.rem(dp + d, n_dp), me)

    pl.semaphore_wait(barrier, n_ctx - 1 + n_dp - 1)

    grads = (ga, gv, gk)

    def on_y(kind, d, to, frm):
        src, dst = grads[kind].at[to], r1.at[kind, frm]
        if d == 0:
            return pltpu.make_async_copy(src, dst, lsem.at[1 + kind])
        return send(src, dst, ysem.at[kind, d], yrem.at[kind, d], dp, x * n_y + to)

    def on_x(kind, d, to, frm):
        dst = ag.at[dp, frm] if kind == 0 else r2.at[kind - 1, frm]
        return send(s1.at[kind, to], dst, xsem.at[kind, d], xrem.at[kind, d], dp, to * n_y + y)

    def q_copy(n, d, to, frm):
        part = width // 2
        src = gq.at[to, :, pl.ds(n * part, part)]
        dst = gq_o.at[:, pl.ds(pl.multiple_of(frm * width + n * part, part), part)]
        if d == 0:
            return pltpu.make_async_copy(src, dst, lsem.at[4 + n])
        return send(src, dst, qsem.at[n, d], qrem.at[n, d], dp, to * n_y + y)

    def hf_copy(i, to, frm):
        return send(
            h.at[:, pl.ds(window(to, share), win)], hf_v.at[frm], hssem.at[i], hrsem.at[i], to, me
        )

    def start_y(kind):
        for d in (*range(1, n_y), 0):
            on_y(kind, d, lax.rem(y + d, n_y), y).start()

    def start_q(n):
        for d in (*range(1, n_x), 0):
            q_copy(n, d, lax.rem(x + d, n_x), x).start()

    def reduce_y(kind):
        on_y(kind, 0, y, y).wait()
        for d in range(1, n_y):
            on_y(kind, d, y, lax.rem(y + n_y - d, n_y)).wait_recv()
        for m in range(n_x):
            total = r1[kind, 0, m].astype(F32)
            for f in range(1, n_y):
                total = total + r1[kind, f, m].astype(F32)
            s1[kind, m] = total.astype(BF16)

    def start_x(kind):
        for d in range(1, n_x):
            on_x(kind, d, lax.rem(x + d, n_x), x).start()

    def arrived_x(kind):
        for d in range(1, n_x):
            on_x(kind, d, x, lax.rem(x + n_x - d, n_x)).wait_recv()

    start_y(0)
    for i, to, frm in hf_pairs(True):
        hf_copy(i, to, dp).start()
    factor = head ** (-0.5)

    @pl.loop(0, n_x)
    def _(m):
        at = pl.ds(pl.multiple_of((m * n_y + y) * rows, rows), rows)
        c, s = cs[at, :], sn[at, :]
        for hd in range(width // head):
            lanes = slice(hd * head, (hd + 1) * head)
            gz = gq_raw[m, hd * rows : (hd + 1) * rows, :] * factor
            u = q_in[m, :, lanes].astype(F32)
            gq[m, :, lanes] = normrope_back(u, gz, qg_ref[...], c, s).astype(BF16)

    start_q(0)
    start_y(1)

    for copy in hf_loads:
        copy.wait()
    for i, _, frm in hf_pairs(False):
        hft[frm] = hf_v[frm].T
    reduce_y(0)
    start_x(0)
    @pl.loop(0, n_ctx)
    def _(i):
        at = pl.ds(pl.multiple_of(i * rows, rows), rows)
        gz = gk_raw[at, :] * factor
        u = k_in[i % n_y, i // n_y].astype(F32)
        gk[i % n_y, i // n_y] = normrope_back(u, gz, kg_ref[...], cs[at, :], sn[at, :]).astype(BF16)

    start_y(2)
    start_q(1)
    ag[dp, x] = s1[0, x]
    arrived_x(0)

    def piece(slot, ch):
        return ag.at[slot, ch]

    def takes(t, ch, way):
        return t <= behind or (t == ahead and (ch < n_x // 2) == (way == 0))

    def ring(slot, ch, way, to):
        return send(piece(slot, ch), piece(slot, ch), ag_s.at[slot, way, ch], ag_r.at[slot, ch], to, me)

    sent = []

    def go(slot, ch, way, to):
        copy = ring(slot, ch, way, to)
        copy.start()
        sent.append(copy)

    for ch in range(n_x):
        if takes(1, ch, 0):
            go(dp, ch, 0, after)
        if takes(1, ch, 1):
            go(dp, ch, 1, before)
    for ch in range(n_x):
        go(dp, ch, 2, twin)

    def relay(t):
        for ch in range(n_x):
            for way, to, hop in ((0, after, n_z - t), (1, before, t)):
                if takes(t, ch, way):
                    slot = lax.rem(z + hop, n_z) * 2 + core
                    ring(slot, ch, way, to).wait_recv()
                    if takes(t + 1, ch, way):
                        go(slot, ch, way, to)
                    go(slot, ch, 2, twin)

    started = [False]

    def weigh(d):
        slots = [lax.rem(z + d, n_z) * 2 + c for c in (core, 1 - core)]
        for ch in range(n_x):
            ring(slots[1], ch, 2, twin).wait_recv()
        a = jnp.concatenate([hft[e] for e in slots], axis=1)
        b = jnp.concatenate(
            [jnp.concatenate([ag[e, hd] for hd in range(n_x)], axis=1) for e in slots], axis=0
        )
        if started[0]:
            dw[...] += dot(a, b)
        else:
            dw[...] = dot(a, b)
            started[0] = True

    model = h_o.shape[1]
    sub = 256

    def hidden_part(n, parts):
        span = model // parts

        @pl.loop(0, span // sub)
        def _(i):
            at = pl.ds(pl.multiple_of(n * span + i * sub, sub), sub)
            h_o[:, at] = dot(vg[...], w_v[at, :], NT).astype(BF16)

    def first_half():
        arrived_x(1)
        for hd in range(n_x):
            vg[:, hd * head : (hd + 1) * head] = r2[0, hd]
        load_w.wait()
        hidden_part(0, 2)

    reduce_y(1)
    start_x(1)
    relay(1)
    reduce_y(2)
    start_x(2)
    r2[0, x] = s1[1, x]
    r2[1, x] = s1[2, x]
    for i, _, frm in hf_pairs(True):
        hf_copy(i, dp, frm).wait_recv()
        hft[frm] = hf_v[frm].T
    for t in range(2, ahead):
        relay(t)
        if t == 2:
            weigh(0)
            first_half()
        else:
            for d in (1, 2) if t == 3 else (t - 1,):
                weigh(d)
                weigh(n_z - d)
    if ahead > 1:
        relay(ahead)
    for d in range(ahead - 1, n_z - ahead + 2) if ahead > 2 else range(n_z):
        weigh(d)
    if ahead < 3:
        first_half()

    off = pl.multiple_of(dp * share - (dp * share) // 128 * 128, 64)
    out_rows = share // n_ctx
    for o in range(0, win - share + 1, 64):

        @pl.when(off == o)
        def _(o=o):
            for c in range(n_ctx):
                at = slice(o + c * out_rows, o + (c + 1) * out_rows)
                dws[c, :out_rows, :] = dw[at, :].astype(BF16)

    def w_copy(d, to, frm):
        return send(dws.at[to], dwr.at[frm], ws.at[d], wr.at[d], dp, to)

    @pl.loop(1, n_ctx)
    def _(d):
        w_copy(d, lax.rem(me + d, n_ctx), me).start()

    dwr[me] = dws[me]
    hidden_part(1, 2)
    arrived_x(2)
    for hd in range(n_x):
        gk_o[:, hd * head : (hd + 1) * head] = r2[1, hd]
    for n in range(2):
        q_copy(n, 0, x, x).wait()
        for d in range(1, n_x):
            q_copy(n, d, x, lax.rem(x + n_x - d, n_x)).wait_recv()
            q_copy(n, d, lax.rem(x + d, n_x), x).wait_send()
    for copy in sent:
        copy.wait_send()
    for kind in range(3):
        for d in range(1, n_y):
            on_y(kind, d, lax.rem(y + d, n_y), y).wait_send()
        for d in range(1, n_x):
            on_x(kind, d, lax.rem(x + d, n_x), x).wait_send()
    for i, to, _ in hf_pairs(True):
        hf_copy(i, to, dp).wait_send()

    @pl.loop(1, n_ctx)
    def _(d):
        w_copy(d, me, lax.rem(me + n_ctx - d, n_ctx)).wait_recv()

    total = dwr[0].astype(F32)
    for c in range(1, n_ctx):
        total = total + dwr[c].astype(F32)
    w_o[...] = total[:out_rows] * (1.0 / (n_dp * n_ctx))

    @pl.loop(1, n_ctx)
    def _(d):
        w_copy(d, lax.rem(me + d, n_ctx), me).wait_send()


def on_device(hidden, queries, key_states, out_grad, w_value, q_gain, k_gain, dest_rows, doc_ids):
    n_dp, n_ctx = lax.axis_size("dp"), lax.axis_size("ctx")
    rows, model = hidden.shape[1:]
    head = q_gain.shape[0]
    kv_width = key_states.shape[2]
    n_x = kv_width // head
    n_y = n_ctx // n_x
    width = queries.shape[2] // n_x
    heads = width // head
    slab = rows * n_ctx
    share = model // n_dp
    win = (share + 127) // 128 * 128
    sizes = (n_dp, n_x, n_y, rows, width, head, share, win)
    sds = jax.ShapeDtypeStruct
    dma = pltpu.SemaphoreType.DMA

    index = jnp.concatenate([dest_rows, doc_ids], axis=0)
    wide = sds((n_x, rows, width), BF16)
    narrow = sds((n_y, n_x, rows, head), BF16)
    half = head // 2
    frequency = rope_base ** (-(np.arange(half, dtype=np.float64) * 2.0 / head))
    frequency = np.concatenate([frequency, frequency])[None]
    low = np.arange(rows, dtype=np.float64)[:, None] * frequency
    table = np.concatenate([np.cos(low), np.sin(low), np.repeat(frequency, 8, axis=0)])
    table = jnp.asarray(table, F32)
    n_docs = 4
    stacked = (n_x, heads * rows, head)
    flat = sds((slab, head), BF16)
    kept = [
        pltpu.with_memory_space_constraint(a, pltpu.HBM)
        for a in (queries[0], out_grad[0], key_states[0], hidden[0], w_value)
    ]
    tail = [
        pltpu.with_memory_space_constraint(a, pltpu.HBM)
        for a in (q_gain[None], k_gain[None], table)
    ]
    q_in, g_in, k_in, index_in, hf, cs, sn, kn, qs, vs = pl.pallas_call(
        functools.partial(arrive_kernel, sizes),
        out_shape=(
            wide,
            wide,
            narrow,
            sds((n_ctx, 2, rows), I32),
            sds((n_dp, rows, win), BF16),
            sds((slab, head), F32),
            sds((slab, head), F32),
            flat,
            sds(stacked, BF16),
            flat,
        ),
        in_specs=[HBM] * 5 + [ANY] + [HBM] * 3,
        out_specs=(VMEM, ANY, VMEM, VMEM, ANY) + (VMEM,) * 5,
        scratch_shapes=[
            pltpu.VMEM((rows, model), BF16),
            pltpu.VMEM((model, kv_width), BF16),
            pltpu.VMEM((rows, kv_width), BF16),
            pltpu.VMEM((n_y, n_x, rows, head), BF16),
            pltpu.VMEM((n_ctx * n_docs, head), F32),
            pltpu.VMEM((n_ctx * n_docs, head), F32),
            pltpu.VMEM((1, head), F32),
            pltpu.VMEM((1, head), F32),
            pltpu.VMEM((2 * rows + 8, head), F32),
            dma((4, n_x)),
            dma((4, n_x)),
            dma((2, n_y)),
            dma((2, n_y)),
            dma((n_ctx,)),
            dma((n_ctx,)),
            dma((n_dp,)),
            dma((n_dp,)),
            dma((11,)),
        ],
        compiler_params=pltpu.CompilerParams(
            collective_id=0, has_side_effects=True, vmem_limit_bytes=24 << 20
        ),
        name="arrive",
    )(*kept, index, *tail)

    tiles = slab // TILE
    gq, gk, gv, ga = pl.pallas_call(
        functools.partial(attend_kernel, (n_x, n_y, rows, heads, head, n_docs)),
        out_shape=(sds(stacked, F32), sds((slab, head), F32), narrow, narrow),
        in_specs=[VMEM] * 5,
        out_specs=(VMEM,) * 4,
        scratch_shapes=[
            pltpu.VMEM(stacked, BF16),
            pltpu.VMEM((tiles, TILE, heads * rows), F32),
            pltpu.VMEM((tiles, TILE, heads * rows), F32),
            pltpu.VMEM((slab, head), F32),
            pltpu.VMEM((head, slab), BF16),
        ],
        compiler_params=pltpu.CompilerParams(vmem_limit_bytes=36 << 20),
        name="attend",
    )(qs, g_in, kn, vs, index_in)

    out_rows = share // n_ctx
    pad = (out_rows + 15) // 16 * 16
    results = (
        sds((rows, n_x * width), BF16),
        sds((rows, kv_width), BF16),
        sds((rows, model), BF16),
        sds((out_rows, kv_width), F32),
    )
    query_grad, key_grad, hidden_grad, weight_grad = pl.pallas_call(
        functools.partial(return_kernel, sizes),
        out_shape=results,
        in_specs=[VMEM] * 2 + [ANY] * 2 + [HBM] * 2 + [ANY] + [VMEM] * 6,
        out_specs=(ANY, VMEM, VMEM, VMEM),
        scratch_shapes=[
            pltpu.VMEM((n_x, rows, width), BF16),
            pltpu.VMEM((n_y, n_x, rows, head), BF16),
            pltpu.VMEM((3, n_y, n_x, rows, head), BF16),
            pltpu.VMEM((3, n_x, rows, head), BF16),
            pltpu.VMEM((2, n_x, rows, head), BF16),
            pltpu.VMEM((rows, kv_width), BF16),
            pltpu.VMEM((n_dp, n_x, rows, head), BF16),
            pltpu.VMEM((model, kv_width), BF16),
            pltpu.VMEM((n_dp, rows, win), BF16),
            pltpu.VMEM((n_dp, win, rows), BF16),
            pltpu.VMEM((win, kv_width), F32),
            pltpu.VMEM((n_ctx, pad, kv_width), BF16),
            pltpu.VMEM((n_ctx, pad, kv_width), BF16),
            dma((2, n_x)),
            dma((2, n_x)),
            dma((3, n_y)),
            dma((3, n_y)),
            dma((3, n_x)),
            dma((3, n_x)),
            dma((6,)),
            dma((n_dp, 3, n_x)),
            dma((n_dp, n_x)),
            dma((n_ctx,)),
            dma((n_ctx,)),
            dma((n_dp,)),
            dma((n_dp,)),
        ],
        compiler_params=pltpu.CompilerParams(
            collective_id=1, has_side_effects=True, vmem_limit_bytes=32 << 20
        ),
        name="give_back",
    )(gq, gk, gv, ga, w_value, hidden[0], hf, q_in, k_in, cs, sn, q_gain[None], k_gain[None])
    return (hidden_grad[None], query_grad[None], key_grad[None], weight_grad)


def solution(mesh):
    rows = P("dp", "ctx", None)
    return jax.shard_map(
        on_device,
        mesh=mesh,
        in_specs=(rows, rows, rows, rows, P(), P(), P(), P("dp", "ctx"), P("dp", "ctx")),
        out_specs=(rows, rows, rows, P(("dp", "ctx"), None)),
        check_vma=False,
    )
```
